32 devices in a mesh: section: 2 (over x), expert: 4 (over y, core), dp: 4 (over z).
Axes of the slice: x: 2, y: 2, z: 4, core: 2. Of those that a mesh axis runs over, the one named last changes fastest.
Arguments:
- arrivals: bfloat16 [2, 1024, 2048], P('section', ('expert', 'dp')), may hold values from -6 to 6
- fresh: bfloat16 [1, 1024, 2048], P(None, ('expert', 'dp')), may hold values from -6 to 6
- routes: int32 [2, 2, 1024, 6], P('section', None, ('expert', 'dp')), may hold values from 0 to 63, as said below
- gates: bfloat16 [2, 2, 1024, 6], P('section', None, ('expert', 'dp')), may hold values from 0.099609375 to 1
- cotangent: bfloat16 [2, 2, 1024, 2048], P('section', None, ('expert', 'dp')), may hold values from -0.3125 to 0.3125
- norm_gain: float32 [2, 2048], P('section'), may hold values from 0.5 to 1.5
- w_gate: bfloat16 [2, 1408, 2048], P('section', 'expert', 'dp'), may hold values from -0.125 to 0.125
- w_up: bfloat16 [2, 1408, 2048], P('section', 'expert', 'dp'), may hold values from -0.125 to 0.125
- w_down: bfloat16 [2, 1408, 2048], P('section', 'expert', 'dp'), may hold values from -0.15625 to 0.15625
Outputs:
- layer_out: bfloat16 [2, 2, 1024, 2048], P('section', None, ('expert', 'dp'))
- grad_down: float32 [2, 1408, 2048], P('section', 'expert', 'dp')
The draws below stay inside these ranges and needn't reach their ends.
Inputs may be any that keep to these rules, and one draw needn't show every extreme that they name: `routes`: each token's 6 entries are different expert numbers.
All inputs are finite; a program needn't handle non-finite values.
Results may differ from the reference program's by a relative error of at most 0.0085.
Values may be sent and summed in bfloat16 or wider, within the bound.
A program may use at most 64 MiB of HBM per device.

```python
import jax
import jax.numpy as jnp
from jax import lax

D = 2048
EXPERTS = 64
TOPK = 6
EXP_HID = 1408
SPLIT = 4
CAP = 12
STEPS = 2
TOK_MB = 64
FLIGHT = 1
HID_DEV = 352
LAYERS = 2
FRESH = 1
TOKENS = 1024


def draw_routes(key, part):
    total_rows = LAYERS * STEPS * TOKENS
    groups = LAYERS * STEPS
    blocks = total_rows // TOK_MB
    key_noise, key_hot, key_rank, key_pick, key_boost = jax.random.split(jax.random.fold_in(key, 7), 5)
    column = jnp.arange(EXPERTS, dtype=jnp.int32)
    noise = jax.random.randint(key_noise, (total_rows, EXPERTS), 0, 1 << 20, dtype=jnp.int32)
    scores = noise * EXPERTS + column[None, :]
    hottest = jax.random.randint(key_hot, (groups,), 0, FLIGHT, dtype=jnp.int32)
    hot_rows = jnp.repeat(hottest, TOKENS)
    ranking = jax.random.randint(key_rank, (blocks, TOK_MB), 0, 1 << 20, dtype=jnp.int32) * TOK_MB + jnp.arange(TOK_MB, dtype=jnp.int32)[None, :]
    ordering = jnp.argsort(jnp.argsort(ranking, axis=1), axis=1).reshape(total_rows)
    forced = (ordering < CAP).astype(jnp.int32)
    scores = scores + forced[:, None] * (column[None, :] == hot_rows[:, None]).astype(jnp.int32) * (1 << 28)
    picked = jax.random.randint(key_pick, (total_rows,), 0, FLIGHT, dtype=jnp.int32)
    boosted = (jax.random.randint(key_boost, (total_rows,), 0, 4, dtype=jnp.int32) == 0).astype(jnp.int32)
    scores = scores + boosted[:, None] * (column[None, :] == picked[:, None]).astype(jnp.int32) * (1 << 27)
    top_values, chosen = lax.top_k(scores, TOPK)
    return chosen.astype(jnp.int32).reshape(LAYERS, STEPS, TOKENS, TOPK)


def level_of(own_key, dims, shards, low, largest):
    level = 1.0
    for dim, blocks in shards:
        draws = jax.random.uniform(jax.random.fold_in(jax.random.fold_in(own_key, 6), dim), (blocks,), jnp.float32, low / len(shards), largest / len(shards))
        level = level * jnp.repeat(jnp.exp(draws), dims[dim] // blocks).reshape((-1,) + (1,) * (len(dims) - 1 - dim))
    return level


def gaussian(rng, extent, width, bound, cuts=(), kind=jnp.bfloat16):
    level = level_of(rng, extent, cuts, -0.22, 0.18) if cuts else 1.0
    values = jax.random.normal(rng, extent, jnp.float32) * width * level
    return jnp.minimum(jnp.maximum(values, -bound), bound).astype(kind)


def setup_inputs(seed: int = 0) -> dict:
    seeds = jax.random.split(jax.random.key(seed), 10)
    return {
        "arrivals": gaussian(seeds[0], (LAYERS, TOKENS, D), 1.0, 6.0, ((0, 2), (1, 16))),
        "fresh": gaussian(seeds[1], (FRESH, TOKENS, D), 1.0, 6.0, ((1, 16),)),
        "routes": draw_routes(jax.random.fold_in(seeds[9], 71), 0),
        "gates": jnp.clip(0.099609375 + 0.9003906 * jax.random.uniform(seeds[3], (LAYERS, STEPS, TOKENS, TOPK), jnp.float32) ** level_of(seeds[3], (LAYERS, STEPS, TOKENS, TOPK), ((0, 2), (2, 16)), -0.2, 0.2), 0.099609375, 1.0).astype(jnp.bfloat16),
        "cotangent": gaussian(seeds[4], (LAYERS, STEPS, TOKENS, D), 0.05, 0.3125, ((0, 2), (2, 16))),
        "norm_gain": jnp.clip(1.0 + 0.1 * jax.random.normal(seeds[5], (LAYERS, D), jnp.float32), 0.5, 1.5),
        "w_gate": gaussian(seeds[6], (LAYERS, FLIGHT * EXP_HID, D), D ** -0.5, 0.125, ((0, 2), (1, 4), (2, 4))),
        "w_up": gaussian(seeds[7], (LAYERS, FLIGHT * EXP_HID, D), D ** -0.5, 0.125, ((0, 2), (1, 4), (2, 4))),
        "w_down": gaussian(seeds[8], (LAYERS, FLIGHT * EXP_HID, D), EXP_HID ** -0.5, 0.15625, ((0, 2), (1, 4), (2, 4))),
    }


def rms_normed(values, gains):
    floats = values.astype(jnp.float32)
    scale = lax.rsqrt(lax.optimization_barrier(jnp.mean(floats * floats, axis=-1, keepdims=True)) + 0.5)
    return (floats * scale * gains[None, :]).astype(jnp.bfloat16)

def layer(inputs, routing, weights, cot, gains, gate_rows, up_rows, down_rows):
    highest = lax.Precision.HIGHEST
    blocks = TOKENS // TOK_MB
    normed = rms_normed(inputs, gains).astype(jnp.float32).reshape(blocks, TOK_MB, D)
    cot_blocks = cot.astype(jnp.float32).reshape(blocks, TOK_MB, D)
    route_blocks = routing.reshape(blocks, TOK_MB, TOPK)
    weight_blocks = weights.astype(jnp.float32).reshape(blocks, TOK_MB, TOPK)
    slot_ids = jnp.arange(CAP, dtype=jnp.int32)
    mixture = jnp.zeros((blocks, TOK_MB, D), jnp.float32)
    grads = []
    for expert in range(FLIGHT):
        matches = route_blocks == expert
        naming = jnp.any(matches, axis=-1).astype(jnp.int32)
        shares = lax.optimization_barrier(jnp.sum(jnp.where(matches, weight_blocks, 0.0), axis=-1))
        places = jnp.cumsum(naming, axis=1) - naming
        select = ((naming[:, None, :] == 1) & (places[:, None, :] == slot_ids[None, :, None])).astype(jnp.float32)
        rows_tok = jnp.einsum('bpt,btd->bpd', select, normed, precision=highest).reshape(blocks * CAP, D)
        rows_cot = jnp.einsum('bpt,btd->bpd', select, cot_blocks, precision=highest).reshape(blocks * CAP, D)
        rows_gate = jnp.einsum('bpt,bt->bp', select, shares, precision=highest)
        first_row = expert * EXP_HID
        gate_w = gate_rows[first_row:first_row + EXP_HID].astype(jnp.float32)
        up_w = up_rows[first_row:first_row + EXP_HID].astype(jnp.float32)
        down_w = down_rows[first_row:first_row + EXP_HID].astype(jnp.float32)
        gate_act = jnp.dot(rows_tok, gate_w.T, precision=highest)
        up_act = jnp.dot(rows_tok, up_w.T, precision=highest)
        hidden = lax.optimization_barrier((jax.nn.silu(gate_act) * up_act).astype(jnp.bfloat16)).astype(jnp.float32)
        pieces = jnp.einsum('rmf,mfd->rmd', hidden.reshape(blocks * CAP, SPLIT, HID_DEV), down_w.reshape(SPLIT, HID_DEV, D), precision=highest)
        pieces = lax.optimization_barrier(pieces.astype(jnp.bfloat16)).astype(jnp.float32)
        expert_out = lax.optimization_barrier(jnp.sum(pieces, axis=1)).reshape(blocks, CAP, D)
        mixture = mixture + jnp.einsum('bpt,bp,bpd->btd', select, rows_gate, expert_out, precision=highest)
        gate_flat = rows_gate.reshape(blocks * CAP)
        weighted = lax.optimization_barrier((hidden * gate_flat[:, None]).astype(jnp.bfloat16)).astype(jnp.float32)
        grads.append(jnp.dot(weighted.T, rows_cot, precision=highest))
    result = (inputs.astype(jnp.float32) + mixture.reshape(TOKENS, D)).astype(jnp.bfloat16)
    return (result, jnp.concatenate(grads, axis=0))

def reference(arrivals, fresh, routes, gates, cotangent, norm_gain, w_gate, w_up, w_down):
    results = []
    grads = []
    for layer_num in range(LAYERS):
        row_out = []
        total = jnp.zeros((FLIGHT * EXP_HID, D), jnp.float32)
        for turn_num in range(STEPS):
            if turn_num == 0:
                inputs = arrivals[layer_num]
            elif layer_num == 0:
                inputs = fresh[turn_num - 1]
            else:
                inputs = results[layer_num - 1][turn_num - 1]
            output, grad_part = layer(inputs, routes[layer_num, turn_num], gates[layer_num, turn_num], cotangent[layer_num, turn_num], norm_gain[layer_num], w_gate[layer_num], w_up[layer_num], w_down[layer_num])
            row_out.append(output)
            total = total + grad_part
        results.append(row_out)
        grads.append(total)
    layer_out = jnp.stack([jnp.stack(row_out) for row_out in results])
    grad_down = jnp.stack(grads)
    return (layer_out, grad_down)
```

```python
import functools

import jax
import jax.numpy as jnp
from jax import lax
from jax.experimental import pallas as pl
from jax.experimental.pallas import tpu as pltpu
from jax.sharding import PartitionSpec as P

SPLIT = 4
CAP = 12
SLOTS = 16
LANES = 128
MESH = pl.DeviceIdType.MESH
BF = jnp.bfloat16
F32 = jnp.float32


def mm(a, b, ca=1, cb=0):
    return lax.dot_general(a, b, (((ca,), (cb,)), ((), ())), preferred_element_type=F32)


def kernel(
    n_s, n_e, n_d, steps,
    arr, fresh, routes, gates, cot, gain, wg, wu, wd,
    out, grad,
    toks, tokr, cots, cotr, parts, partr, hid, rets, retr,
    base, inc, place_s, place_r, rows_s, rows_r,
    send_sems, recv_sems,
):
    sec = lax.axis_index("section")
    exp = lax.axis_index("expert")
    dp = lax.axis_index("dp")
    group = n_e * n_d
    flight = n_e // SPLIT
    tok_rows, width = arr.shape[1], arr.shape[2]
    cols = width // n_d
    chunk = CAP * group // n_d
    used = flight * SLOTS
    compact = used < tok_rows
    me = exp * n_d + dp
    nxt = lax.rem(sec + 1, n_s)

    def each(count, body):
        if count <= 32:
            for i in range(1, count):
                body(i)
        else:
            @pl.loop(1, count)
            def _(i):
                body(i)

    def member(off):
        g = lax.rem(me + off, group)
        return g, g // n_d, lax.rem(g, n_d)

    barrier = pltpu.get_barrier_semaphore()

    def greet(off):
        _, te, td = member(off)
        pl.semaphore_signal(barrier, inc=1, device_id=(sec, te, td), device_id_type=MESH)

    each(group, greet)
    greeted = group - 1
    sections = {off for off in (1 % n_s, (n_s - 1) % n_s) if off}
    for off in sorted(sections):
        pl.semaphore_signal(
            barrier, inc=1, device_id=(lax.rem(sec + off, n_s), exp, dp), device_id_type=MESH
        )
        greeted += 1

    def remote(src, dst, k, phase, target):
        return pltpu.make_async_remote_copy(
            src_ref=src, dst_ref=dst, send_sem=send_sems.at[k, phase],
            recv_sem=recv_sems.at[k, phase], device_id=target, device_id_type=MESH,
        )

    def wait_all(ref, k, phase, send=False):
        copy = remote(ref, ref, k, phase, (sec, exp, dp))
        if send:
            copy.wait_send()
        else:
            copy.wait_recv()

    lane = lax.broadcasted_iota(jnp.int32, (tok_rows, LANES), 1)
    lane_expert = lane >> 4
    lane_slot = lane & (SLOTS - 1)
    t_row = lax.broadcasted_iota(jnp.int32, (tok_rows, tok_rows), 0)
    t_col = lax.broadcasted_iota(jnp.int32, (tok_rows, tok_rows), 1)
    before = jnp.where(t_col < t_row, 1.0, 0.0).astype(BF)

    def selection(k):
        routing = routes[0, k]
        weights = gates[0, k].astype(F32)
        naming = jnp.zeros((tok_rows, LANES), F32)
        shares = jnp.zeros((tok_rows, LANES), F32)
        for j in range(routing.shape[1]):
            hit = routing[:, j:j + 1] == lane_expert
            naming = jnp.where(hit, 1.0, naming)
            shares = shares + jnp.where(hit, weights[:, j:j + 1], 0.0)
        places = mm(before, naming.astype(BF))
        chosen = jnp.where(places == lane_slot.astype(F32), naming, 0.0)
        chosen = jnp.where(lane_slot < CAP, chosen, 0.0)
        chosen = jnp.where(lane_expert < flight, chosen, 0.0)
        sel = chosen.T[:used].astype(BF)
        slot_gate = jnp.sum((chosen * shares).T, axis=1, keepdims=True)[:used]
        return chosen, sel, slot_gate

    picks = [selection(k) for k in range(steps)]

    r_i = lax.broadcasted_iota(jnp.int32, (CAP * group, SLOTS * group), 0)
    c_i = lax.broadcasted_iota(jnp.int32, (CAP * group, SLOTS * group), 1)
    c_slot = c_i & (SLOTS - 1)
    squeeze = jnp.where(r_i == (c_i >> 4) * CAP + c_slot, 1.0, 0.0)
    squeeze = jnp.where(c_slot < CAP, squeeze, 0.0).astype(BF)

    def fill_rows(store, k, rows):
        for d in range(n_d):
            for f in range(flight):
                store[k, d, f] = rows[f * SLOTS:(f + 1) * SLOTS, d * cols:(d + 1) * cols]

    def spread(store, landing, k, phase):
        def one(off):
            _, te, td = member(off)
            remote(store.at[k, td, te // SPLIT], landing.at[k, me], k, phase, (sec, te, td)).start()

        each(group, one)
        landing[k, me] = store[k, dp, exp // SPLIT]

    def load_in(k):
        return arr[0] if k == 0 else inc[k]

    def tok_phase(k):
        rows = mm(picks[k][1], load_in(k))
        scale = lax.rsqrt(jnp.mean(rows * rows, axis=1, keepdims=True) + 0.5)
        fill_rows(toks, k, (rows * scale * gain[...]).astype(BF))

    def cot_phase(k):
        chosen, sel, slot_gate = picks[k]
        fill_rows(cots, k, (mm(sel, cot[0, k]) * slot_gate).astype(BF))
        spread(cots, cotr, k, 1)

    for k in range(steps):
        chosen, sel, slot_gate = picks[k]
        tok_phase(k)
        if k == 0:
            pl.semaphore_wait(barrier, greeted)
        spread(toks, tokr, k, 0)
        if n_s > 1 and compact and k < steps - 1:
            place_s[k] = chosen.astype(BF)
            remote(place_s.at[k], place_r.at[k], k, 5, (nxt, exp, dp)).start()
            source = arr.at[0] if k == 0 else inc.at[k]
            remote(source, base.at[k], k, 6, (nxt, exp, dp)).start()
        if k == 0:
            cot_phase(0)

        wait_all(tokr.at[k, pl.ds(0, group - 1)], k, 0)
        tok = mm(squeeze, tokr[k].reshape(group * SLOTS, cols)).astype(BF)
        part_g = mm(tok, wg[0], 1, 1)
        part_u = mm(tok, wu[0], 1, 1)
        for d in range(n_d):
            parts[k, d, 0] = part_g[d * chunk:(d + 1) * chunk].astype(BF)
            parts[k, d, 1] = part_u[d * chunk:(d + 1) * chunk].astype(BF)
        for off in range(1, n_d):
            td = lax.rem(dp + off, n_d)
            remote(parts.at[k, td], partr.at[k, dp], k, 2, (sec, exp, td)).start()
        partr[k, dp] = parts[k, dp]
        wait_all(partr.at[k, pl.ds(0, n_d - 1)], k, 2)
        act_g = sum(partr[k, d, 0].astype(F32) for d in range(n_d))
        act_u = sum(partr[k, d, 1].astype(F32) for d in range(n_d))
        hid[k, dp] = (act_g / (1.0 + jnp.exp(-act_g)) * act_u).astype(BF)
        for off in range(1, n_d):
            td = lax.rem(dp + off, n_d)
            remote(hid.at[k, dp], hid.at[k, dp], k, 3, (sec, exp, td)).start()
        wait_all(hid.at[k, pl.ds(0, n_d - 1)], k, 3)
        hidden = hid[k].reshape(n_d * chunk, wg.shape[1])
        wide = mm(squeeze, hidden, 0, 0).astype(BF)
        rets[k] = mm(wide, wd[0]).astype(BF).reshape(group, SLOTS, cols)

        def give_back(off):
            g, te, td = member(off)
            remote(rets.at[k, g], retr.at[k, exp, dp], k, 4, (sec, te, td)).start()

        each(group, give_back)
        retr[k, exp, dp] = rets[k, me]
        if k + 1 < steps:
            cot_phase(k + 1)
        wait_all(cotr.at[k, pl.ds(0, group - 1)], k, 1)
        part = mm(wide, cotr[k].reshape(group * SLOTS, cols), 0, 0)
        grad[0] = part if k == 0 else grad[0] + part

        wait_all(rets.at[k, pl.ds(0, group - 1)], k, 4)
        pieces = []
        for f in range(flight):
            blocks = []
            for d in range(n_d):
                total = retr[k, f * SPLIT, d].astype(F32)
                for j in range(1, SPLIT):
                    total = total + retr[k, f * SPLIT + j, d].astype(F32)
                blocks.append(total)
            pieces.append(jnp.concatenate(blocks, axis=1))
        mixed = (jnp.concatenate(pieces, axis=0) if flight > 1 else pieces[0]) * slot_gate
        high = mixed.astype(BF)
        low = (mixed - high.astype(F32)).astype(BF)
        spot = chosen[:, :used].astype(BF)
        mixture = mm(spot, high) + mm(spot, low)
        result = (load_in(k).astype(F32) + mixture).astype(BF)
        out[0, k] = result
        if k + 1 < steps:
            if n_s == 1:
                inc[k + 1] = fresh[k]
            elif compact:
                rows_s[k] = mm(sel, result).astype(BF)
                remote(rows_s.at[k], rows_r.at[k], k, 7, (nxt, exp, dp)).start()
                wait_all(base.at[k], k, 6)
                wait_all(place_r.at[k], k, 5)
                wait_all(rows_r.at[k], k, 7)
                before_sel = place_r[k][:, :used].astype(F32)
                if flight > 1:
                    u_row = lax.broadcasted_iota(jnp.int32, (used, used), 0) >> 4
                    u_col = lax.broadcasted_iota(jnp.int32, (used, used), 1) >> 4
                    earlier = jnp.where(u_row < u_col, 1.0, 0.0).astype(BF)
                    before_sel = jnp.where(mm(before_sel.astype(BF), earlier) > 0.5, 0.0, before_sel)
                kept = jnp.sum(before_sel, axis=1, keepdims=True)
                moved = base[k].astype(F32) * (1.0 - kept) + mm(before_sel.astype(BF), rows_r[k])
                inc[k + 1] = jnp.where(sec == 0, fresh[k].astype(F32), moved).astype(BF)
            else:
                remote(out.at[0, k], base.at[k], k, 6, (nxt, exp, dp)).start()
                wait_all(base.at[k], k, 6)
                inc[k + 1] = jnp.where(
                    sec == 0, fresh[k].astype(F32), base[k].astype(F32)
                ).astype(BF)

    for k in range(steps):
        wait_all(tokr.at[k, pl.ds(0, group - 1)], k, 0, True)
        wait_all(cotr.at[k, pl.ds(0, group - 1)], k, 1, True)
        wait_all(parts.at[k, pl.ds(0, n_d - 1)], k, 2, True)
        wait_all(hid.at[k, pl.ds(0, n_d - 1)], k, 3, True)
        wait_all(rets.at[k, pl.ds(0, group - 1)], k, 4, True)
        if n_s > 1 and k < steps - 1:
            wait_all(base.at[k], k, 6, True)
            if compact:
                wait_all(place_s.at[k], k, 5, True)
                wait_all(rows_s.at[k], k, 7, True)


def local(sizes, arrivals, fresh, routes, gates, cotangent, norm_gain, w_gate, w_up, w_down):
    n_s, n_e, n_d = sizes
    steps = routes.shape[1]
    tok_rows, width = arrivals.shape[1:]
    units, cols = w_gate.shape[1:]
    flight = n_e // SPLIT
    group = n_e * n_d
    chunk = CAP * group // n_d
    used = flight * SLOTS
    hops = max(steps - 1, 1)
    vmem = pl.BlockSpec(memory_space=pltpu.VMEM)
    return pl.pallas_call(
        functools.partial(kernel, n_s, n_e, n_d, steps),
        out_shape=(
            jax.ShapeDtypeStruct((1, steps, tok_rows, width), BF),
            jax.ShapeDtypeStruct((1, units, cols), F32),
        ),
        in_specs=[vmem] * 9,
        out_specs=(vmem, vmem),
        scratch_shapes=[
            pltpu.VMEM((steps, n_d, flight, SLOTS, cols), BF),
            pltpu.VMEM((steps, group, SLOTS, cols), BF),
            pltpu.VMEM((steps, n_d, flight, SLOTS, cols), BF),
            pltpu.VMEM((steps, group, SLOTS, cols), BF),
            pltpu.VMEM((steps, n_d, 2, chunk, units), BF),
            pltpu.VMEM((steps, n_d, 2, chunk, units), BF),
            pltpu.VMEM((steps, n_d, chunk, units), BF),
            pltpu.VMEM((steps, group, SLOTS, cols), BF),
            pltpu.VMEM((steps, n_e, n_d, SLOTS, cols), BF),
            pltpu.VMEM((hops, tok_rows, width), BF),
            pltpu.VMEM((steps, tok_rows, width), BF),
            pltpu.VMEM((hops, tok_rows, LANES), BF),
            pltpu.VMEM((hops, tok_rows, LANES), BF),
            pltpu.VMEM((hops, used, width), BF),
            pltpu.VMEM((hops, used, width), BF),
            pltpu.SemaphoreType.DMA((steps, 8)),
            pltpu.SemaphoreType.DMA((steps, 8)),
        ],
        compiler_params=pltpu.CompilerParams(
            collective_id=0, has_side_effects=True, vmem_limit_bytes=60000 * 1024
        ),
    )(arrivals, fresh, routes, gates, cotangent, norm_gain, w_gate, w_up, w_down)


def solution(mesh):
    placed = (
        P("section", ("expert", "dp"), None),
        P(None, ("expert", "dp"), None),
        P("section", None, ("expert", "dp"), None),
        P("section", None, ("expert", "dp"), None),
        P("section", None, ("expert", "dp"), None),
        P("section", None),
        P("section", "expert", "dp"),
        P("section", "expert", "dp"),
        P("section", "expert", "dp"),
    )
    sizes = (mesh.shape["section"], mesh.shape["expert"], mesh.shape["dp"])
    return jax.shard_map(
        functools.partial(local, sizes),
        mesh=mesh,
        in_specs=placed,
        out_specs=(P("section", None, ("expert", "dp"), None), P("section", "expert", "dp")),
        check_vma=False,
    )
```

```python
import functools

import jax
import jax.numpy as jnp
from jax import lax
from jax.experimental import pallas as pl
from jax.experimental.pallas import tpu as pltpu
from jax.sharding import PartitionSpec as P

SPLIT = 4
CAP = 12
SLOTS = 16
CORES = 2
MESH = pl.DeviceIdType.MESH
BF = jnp.bfloat16
F32 = jnp.float32


def mm(a, b, ca=1, cb=0):
    return lax.dot_general(a, b, (((ca,), (cb,)), ((), ())), preferred_element_type=F32)


def kernel(
    n_s, n_e, n_d, steps,
    arr, fresh, routes, gates, cot, gain, wg, wu, wd,
    out, grad,
    toks, tokr, cots, cotr, parts, partr, hid, rets, pair, rsum, retr,
    base, inc, place_s, place_r, rows_s, rows_r,
    send_sems, recv_sems,
):
    sec = lax.axis_index("section")
    exp = lax.axis_index("expert")
    dp = lax.axis_index("dp")
    chips = n_e * n_d // CORES
    group = CORES * chips
    flight = n_e // SPLIT
    tok_rows, width = arr.shape[1], arr.shape[2]
    cols = width // n_d
    half = cols // 2
    wide_cols = cols + half
    chunk = CAP * group // n_d
    used = flight * SLOTS
    compact = used < tok_rows
    core = lax.rem(exp, CORES)
    chip = (exp // CORES) * n_d + dp
    sibling = (sec, exp + 1 - 2 * core, dp)
    nxt = lax.rem(sec + 1, n_s)

    def each(count, body):
        if count <= 32:
            for i in range(1, count):
                body(i)
        else:
            @pl.loop(1, count)
            def _(i):
                body(i)

    def member(off):
        q = lax.rem(chip + off, chips)
        return q, (q // n_d) * CORES + core, lax.rem(q, n_d)

    barrier = pltpu.get_barrier_semaphore()

    def signal(target):
        pl.semaphore_signal(barrier, inc=1, device_id=target, device_id_type=MESH)

    def greet(off):
        _, te, td = member(off)
        signal((sec, te, td))

    each(chips, greet)
    signal(sibling)
    greeted = chips
    for off in sorted({off for off in (1 % n_s, (n_s - 1) % n_s) if off}):
        signal((lax.rem(sec + off, n_s), exp, dp))
        greeted += 1

    def remote(src, dst, k, phase, target):
        return pltpu.make_async_remote_copy(
            src_ref=src, dst_ref=dst, send_sem=send_sems.at[k, phase],
            recv_sem=recv_sems.at[k, phase], device_id=target, device_id_type=MESH,
        )

    def wait_all(ref, k, phase, send=False):
        copy = remote(ref, ref, k, phase, sibling)
        if send:
            copy.wait_send()
        else:
            copy.wait_recv()

    lane = lax.broadcasted_iota(jnp.int32, (used, tok_rows), 0)
    lane_expert = lane >> 4
    lane_slot = lane & (SLOTS - 1)
    t_row = lax.broadcasted_iota(jnp.int32, (tok_rows, tok_rows), 0)
    t_col = lax.broadcasted_iota(jnp.int32, (tok_rows, tok_rows), 1)
    earlier_tok = jnp.where(t_row < t_col, 1.0, 0.0).astype(BF)

    def selection(k):
        naming = jnp.zeros((used, tok_rows), F32)
        shares = jnp.zeros((used, tok_rows), F32)
        for j in range(routes.shape[1]):
            hit = routes[0, j, k:k + 1, :] == lane_expert
            naming = jnp.where(hit, 1.0, naming)
            shares = shares + jnp.where(hit, gates[0, j].astype(F32)[k:k + 1, :], 0.0)
        places = mm(naming.astype(BF), earlier_tok)
        chosen = jnp.where(places == lane_slot.astype(F32), naming, 0.0)
        chosen = jnp.where(lane_slot < CAP, chosen, 0.0)
        slot_gate = jnp.sum(chosen * shares, axis=1, keepdims=True)
        return chosen.astype(BF), slot_gate

    picks = [selection(k) for k in range(steps)]

    r_i = lax.broadcasted_iota(jnp.int32, (CAP * group, 8 * group), 0)
    c_i = lax.broadcasted_iota(jnp.int32, (CAP * group, 8 * group), 1)
    c_slot = c_i & 7
    shift = r_i - (c_i >> 3) * CAP - c_slot
    low_rows = jnp.where(shift == 0, 1.0, 0.0).astype(BF)
    tail_a = jnp.where((shift == 8) & (c_slot < 4), 1.0, 0.0).astype(BF)
    tail_b = jnp.where((shift == 4) & (c_slot >= 4), 1.0, 0.0).astype(BF)

    def swap(block):
        return jnp.concatenate([block[4:], block[:4]], axis=0)

    def fill_rows(store, k, rows):
        for f in range(flight):
            top = rows[f * SLOTS:f * SLOTS + 8]
            bottom = rows[f * SLOTS + 8:(f + 1) * SLOTS]
            for d in range(n_d):
                at = d * cols
                store[k, d, f, :, :cols] = top[:, at:at + cols].astype(BF)
                store[k, d, f, :, cols:] = (
                    bottom[:, at:at + half] + swap(bottom[:, at + half:at + cols])
                ).astype(BF)

    def unpack(landing, k):
        flat = landing[k].reshape(group * 8, wide_cols)
        tail = flat[:, cols:]
        return jnp.concatenate(
            [
                mm(low_rows, flat[:, :half]) + mm(tail_a, tail),
                mm(low_rows, flat[:, half:cols]) + mm(tail_b, tail),
            ],
            axis=1,
        ).astype(BF)

    def spread(store, landing, k, phase):
        def one(off):
            _, te, td = member(off)
            remote(
                store.at[k, td, te // SPLIT], landing.at[k, core, chip], k, phase, (sec, te, td)
            ).start()

        each(chips, one)
        landing[k, core, chip] = store[k, dp, exp // SPLIT]

    def pass_on(landing, k, phase):
        wait_all(landing.at[k, 0, pl.ds(0, chips - 1)], k, phase)
        remote(landing.at[k, core], landing.at[k, core], k, phase + 1, sibling).start()

    def load_in(k):
        return arr[0] if k == 0 else inc[k]

    def tok_phase(k):
        rows = mm(picks[k][0], load_in(k))
        scale = lax.rsqrt(jnp.mean(rows * rows, axis=1, keepdims=True) + 0.5)
        fill_rows(toks, k, rows * scale * gain[...])

    for k in range(steps):
        sel, slot_gate = picks[k]
        tok_phase(k)
        if k == 0:
            pl.semaphore_wait(barrier, greeted)
        spread(toks, tokr, k, 0)
        if n_s > 1 and compact and k < steps - 1:
            place_s[k] = sel
            remote(place_s.at[k], place_r.at[k], k, 8, (nxt, exp, dp)).start()
            source = arr.at[0] if k == 0 else inc.at[k]
            remote(source, base.at[k], k, 9, (nxt, exp, dp)).start()
        if k == 0:
            for turn in range(steps):
                pick, share = picks[turn]
                fill_rows(cots, turn, mm(pick, cot[0, turn]) * share)
                spread(cots, cotr, turn, 2)

        pass_on(tokr, k, 0)
        wait_all(tokr.at[k, 0], k, 1)
        tok = unpack(tokr, k)
        part_g = mm(tok, wg[0], 1, 1)
        part_u = mm(tok, wu[0], 1, 1)
        for d in range(n_d):
            parts[k, d, 0] = part_g[d * chunk:(d + 1) * chunk].astype(BF)
            parts[k, d, 1] = part_u[d * chunk:(d + 1) * chunk].astype(BF)
        for off in range(1, n_d):
            td = lax.rem(dp + off, n_d)
            remote(parts.at[k, td], partr.at[k, dp], k, 4, (sec, exp, td)).start()
        partr[k, dp] = parts[k, dp]
        pass_on(cotr, k, 2)
        wait_all(partr.at[k, pl.ds(0, n_d - 1)], k, 4)
        act_g = sum(partr[k, d, 0].astype(F32) for d in range(n_d))
        act_u = sum(partr[k, d, 1].astype(F32) for d in range(n_d))
        hid[k, dp] = (act_g / (1.0 + jnp.exp(-act_g)) * act_u).astype(BF)
        for off in range(1, n_d):
            td = lax.rem(dp + off, n_d)
            remote(hid.at[k, dp], hid.at[k, dp], k, 5, (sec, exp, td)).start()
        wait_all(hid.at[k, pl.ds(0, n_d - 1)], k, 5)
        hidden = hid[k].reshape(n_d * chunk, wg.shape[1])
        piece = mm(hidden, wd[0]).astype(BF)
        rets[k, :, :, :, :cols] = mm(low_rows, piece, 0, 0).astype(BF).reshape(
            CORES, chips, 8, cols
        )
        rets[k, :, :, :, cols:] = (
            mm(tail_a, piece[:, :half], 0, 0) + mm(tail_b, piece[:, half:], 0, 0)
        ).astype(BF).reshape(CORES, chips, 8, half)

        remote(rets.at[k, 1 - core], pair.at[k], k, 6, sibling).start()
        wait_all(pair.at[k], k, 6)
        rsum[k] = (rets[k, core].astype(F32) + pair[k].astype(F32)).astype(BF)

        def give_back(off):
            q, te, td = member(off)
            remote(rsum.at[k, q], retr.at[k, exp // CORES, dp], k, 7, (sec, te, td)).start()

        each(chips, give_back)
        retr[k, exp // CORES, dp] = rsum[k, chip]
        wait_all(cotr.at[k, 0], k, 3)
        part = mm(hidden, unpack(cotr, k), 0, 0)
        grad[0] = part if k == 0 else grad[0] + part

        wait_all(rsum.at[k, pl.ds(0, chips - 1)], k, 7)
        tops = []
        row_8 = lax.broadcasted_iota(jnp.int32, (8, half), 0)
        pairs = SPLIT // CORES
        for f in range(flight):
            top, tail = [], []
            for d in range(n_d):
                total = sum(retr[k, f * pairs + j, d].astype(F32) for j in range(pairs))
                top.append(total[:, :cols])
                last = total[:, cols:]
                tail.append(jnp.where(row_8 < 4, last, 0.0))
                tail.append(jnp.where(row_8 < 4, swap(last), 0.0))
            tops.append(jnp.concatenate(top, axis=1))
            tops.append(jnp.concatenate(tail, axis=1))
        mixed = jnp.concatenate(tops, axis=0) * slot_gate
        high = mixed.astype(BF)
        low = (mixed - high.astype(F32)).astype(BF)
        mixture = mm(sel, high, 0, 0) + mm(sel, low, 0, 0)
        result = (load_in(k).astype(F32) + mixture).astype(BF)
        out[0, k] = result
        if k + 1 < steps:
            if n_s == 1:
                inc[k + 1] = fresh[k]
            elif compact:
                rows_s[k] = mm(sel, result).astype(BF)
                remote(rows_s.at[k], rows_r.at[k], k, 10, (nxt, exp, dp)).start()
                wait_all(base.at[k], k, 9)
                wait_all(place_r.at[k], k, 8)
                wait_all(rows_r.at[k], k, 10)
                spot = place_r[k]
                if flight > 1:
                    u_row = lax.broadcasted_iota(jnp.int32, (used, used), 0) >> 4
                    u_col = lax.broadcasted_iota(jnp.int32, (used, used), 1) >> 4
                    sooner = jnp.where(u_col < u_row, 1.0, 0.0).astype(BF)
                    spot = jnp.where(mm(sooner, spot) > 0.5, 0.0, spot.astype(F32)).astype(BF)
                kept = mm(spot, jnp.ones((used, width), BF), 0, 0)
                moved = jnp.where(kept > 0.5, mm(spot, rows_r[k], 0, 0), base[k].astype(F32))
                inc[k + 1] = jnp.where(sec == 0, fresh[k].astype(F32), moved).astype(BF)
            else:
                remote(out.at[0, k], base.at[k], k, 9, (nxt, exp, dp)).start()
                wait_all(base.at[k], k, 9)
                inc[k + 1] = jnp.where(
                    sec == 0, fresh[k].astype(F32), base[k].astype(F32)
                ).astype(BF)

    for k in range(steps):
        wait_all(tokr.at[k, 0, pl.ds(0, chips - 1)], k, 0, True)
        wait_all(tokr.at[k, 0], k, 1, True)
        wait_all(cotr.at[k, 0, pl.ds(0, chips - 1)], k, 2, True)
        wait_all(cotr.at[k, 0], k, 3, True)
        wait_all(parts.at[k, pl.ds(0, n_d - 1)], k, 4, True)
        wait_all(hid.at[k, pl.ds(0, n_d - 1)], k, 5, True)
        wait_all(pair.at[k], k, 6, True)
        wait_all(rsum.at[k, pl.ds(0, chips - 1)], k, 7, True)
        if n_s > 1 and k < steps - 1:
            wait_all(base.at[k], k, 9, True)
            if compact:
                wait_all(place_s.at[k], k, 8, True)
                wait_all(rows_s.at[k], k, 10, True)


def local(sizes, arrivals, fresh, routes, gates, cotangent, norm_gain, w_gate, w_up, w_down):
    n_s, n_e, n_d = sizes
    steps = routes.shape[1]
    tok_rows, width = arrivals.shape[1:]
    units, cols = w_gate.shape[1:]
    flight = n_e // SPLIT
    chips = n_e * n_d // CORES
    chunk = CAP * n_e
    used = flight * SLOTS
    hops = max(steps - 1, 1)
    packed = cols + cols // 2
    vmem = pl.BlockSpec(memory_space=pltpu.VMEM)
    return pl.pallas_call(
        functools.partial(kernel, n_s, n_e, n_d, steps),
        out_shape=(
            jax.ShapeDtypeStruct((1, steps, tok_rows, width), BF),
            jax.ShapeDtypeStruct((1, units, cols), F32),
        ),
        in_specs=[vmem] * 9,
        out_specs=(vmem, vmem),
        scratch_shapes=[
            pltpu.VMEM((steps, n_d, flight, 8, packed), BF),
            pltpu.VMEM((steps, CORES, chips, 8, packed), BF),
            pltpu.VMEM((steps, n_d, flight, 8, packed), BF),
            pltpu.VMEM((steps, CORES, chips, 8, packed), BF),
            pltpu.VMEM((steps, n_d, 2, chunk, units), BF),
            pltpu.VMEM((steps, n_d, 2, chunk, units), BF),
            pltpu.VMEM((steps, n_d, chunk, units), BF),
            pltpu.VMEM((steps, CORES, chips, 8, packed), BF),
            pltpu.VMEM((steps, chips, 8, packed), BF),
            pltpu.VMEM((steps, chips, 8, packed), BF),
            pltpu.VMEM((steps, n_e // CORES, n_d, 8, packed), BF),
            pltpu.VMEM((hops, tok_rows, width), BF),
            pltpu.VMEM((steps, tok_rows, width), BF),
            pltpu.VMEM((hops, used, tok_rows), BF),
            pltpu.VMEM((hops, used, tok_rows), BF),
            pltpu.VMEM((hops, used, width), BF),
            pltpu.VMEM((hops, used, width), BF),
            pltpu.SemaphoreType.DMA((steps, 11)),
            pltpu.SemaphoreType.DMA((steps, 11)),
        ],
        compiler_params=pltpu.CompilerParams(
            collective_id=0, has_side_effects=True, vmem_limit_bytes=60000 * 1024
        ),
    )(
        arrivals, fresh, jnp.transpose(routes, (0, 3, 1, 2)),
        jnp.transpose(gates, (0, 3, 1, 2)), cotangent,
        norm_gain, w_gate, w_up, w_down,
    )


def solution(mesh):
    placed = (
        P("section", ("expert", "dp"), None),
        P(None, ("expert", "dp"), None),
        P("section", None, ("expert", "dp"), None),
        P("section", None, ("expert", "dp"), None),
        P("section", None, ("expert", "dp"), None),
        P("section", None),
        P("section", "expert", "dp"),
        P("section", "expert", "dp"),
        P("section", "expert", "dp"),
    )
    sizes = (mesh.shape["section"], mesh.shape["expert"], mesh.shape["dp"])
    return jax.shard_map(
        functools.partial(local, sizes),
        mesh=mesh,
        in_specs=placed,
        out_specs=(P("section", None, ("expert", "dp"), None), P("section", "expert", "dp")),
        check_vma=False,
    )
```

```python
import functools

import jax
import jax.numpy as jnp
from jax import lax
from jax.experimental import pallas as pl
from jax.experimental.pallas import tpu as pltpu
from jax.sharding import PartitionSpec as P

SPLIT = 4
CAP = 12
SLOTS = 16
CORES = 2
MESH = pl.DeviceIdType.MESH
BF = jnp.bfloat16
F32 = jnp.float32


def mm(a, b, ca=1, cb=0):
    return lax.dot_general(a, b, (((ca,), (cb,)), ((), ())), preferred_element_type=F32)


def kernel(
    n_s, n_e, n_d, steps,
    arr_h, fresh_h, routes_h, gates_h, cot_h, gain_h, wg_h, wu_h, wd_h,
    out, grad,
    fresh, routes, gates, cot, gain, wg, wu, wd, load_sems,
    toks, tokr, cots, cotr, parts, partr, hid, rets, pair, rsum, retr,
    base, inc, place_s, place_r, rows_s, rows_r,
    send_sems, recv_sems,
):
    sec = lax.axis_index("section")
    exp = lax.axis_index("expert")
    dp = lax.axis_index("dp")
    chips = n_e * n_d // CORES
    group = CORES * chips
    flight = n_e // SPLIT
    tok_rows, width = inc.shape[1:]
    cols = width // n_d
    half = cols // 2
    wide_cols = cols + half
    chunk = CAP * group // n_d
    used = flight * SLOTS
    compact = used < tok_rows
    core = lax.rem(exp, CORES)
    chip = (exp // CORES) * n_d + dp
    sibling = (sec, exp + 1 - 2 * core, dp)
    nxt = lax.rem(sec + 1, n_s)

    def far(j):
        low = n_d - 1 - j - (dp + j) // max(n_d - 1, 1)
        high = j + (j - dp + n_d) // n_d
        up = dp // ((n_d + 1) // 2)
        return up * high + (1 - up) * low

    n_y = n_e // CORES
    mine_y = exp // CORES

    def each(body):
        def far_one(i):
            body((mine_y + 1 + lax.rem(i, n_y)) % n_y, far(i // n_y))

        if chips <= 32:
            for i in range((n_d - 1) * n_y):
                body((mine_y + 1 + i % n_y) % n_y, far(i // n_y))
        else:
            @pl.loop(0, (n_d - 1) * n_y)
            def _(i):
                far_one(i)
        for o in range(1, n_y):
            body((mine_y + o) % n_y, dp)

    barrier = pltpu.get_barrier_semaphore()

    def signal(target):
        pl.semaphore_signal(barrier, inc=1, device_id=target, device_id_type=MESH)

    each(lambda ty, td: signal((sec, ty * CORES + core, td)))
    signal(sibling)
    greeted = chips
    for off in sorted({off for off in (1 % n_s, (n_s - 1) % n_s) if off}):
        signal((lax.rem(sec + off, n_s), exp, dp))
        greeted += 1

    loads = [
        pltpu.make_async_copy(src, dst, load_sems.at[i])
        for i, (src, dst) in enumerate((
            (routes_h, routes), (gates_h, gates), (gain_h, gain), (arr_h.at[0], inc.at[0]),
            (cot_h, cot), (wg_h, wg), (wu_h, wu), (wd_h, wd), (fresh_h, fresh),
        ))
    ]
    for load in loads:
        load.start()

    def remote(src, dst, k, phase, target):
        return pltpu.make_async_remote_copy(
            src_ref=src, dst_ref=dst, send_sem=send_sems.at[k, phase],
            recv_sem=recv_sems.at[k, phase], device_id=target, device_id_type=MESH,
        )

    def wait_all(ref, k, phase, send=False):
        copy = remote(ref, ref, k, phase, sibling)
        if send:
            copy.wait_send()
        else:
            copy.wait_recv()

    for load in loads[:3]:
        load.wait()

    lane = lax.broadcasted_iota(jnp.int32, (used, tok_rows), 0)
    lane_expert = lane >> 4
    lane_slot = lane & (SLOTS - 1)
    t_row = lax.broadcasted_iota(jnp.int32, (tok_rows, tok_rows), 0)
    t_col = lax.broadcasted_iota(jnp.int32, (tok_rows, tok_rows), 1)
    earlier_tok = jnp.where(t_row < t_col, 1.0, 0.0).astype(BF)

    def selection(k):
        naming = jnp.zeros((used, tok_rows), F32)
        shares = jnp.zeros((used, tok_rows), F32)
        for j in range(routes.shape[1]):
            hit = routes[0, j, k:k + 1, :] == lane_expert
            naming = jnp.where(hit, 1.0, naming)
            shares = shares + jnp.where(hit, gates[0, j].astype(F32)[k:k + 1, :], 0.0)
        places = mm(naming.astype(BF), earlier_tok)
        chosen = jnp.where(places == lane_slot.astype(F32), naming, 0.0)
        chosen = jnp.where(lane_slot < CAP, chosen, 0.0)
        slot_gate = jnp.sum(chosen * shares, axis=1, keepdims=True)
        return chosen.astype(BF), slot_gate

    picks = [selection(k) for k in range(steps)]

    r_i = lax.broadcasted_iota(jnp.int32, (CAP * group, 8 * group), 0)
    c_i = lax.broadcasted_iota(jnp.int32, (CAP * group, 8 * group), 1)
    c_slot = c_i & 7
    shift = r_i - (c_i >> 3) * CAP - c_slot
    low_rows = jnp.where(shift == 0, 1.0, 0.0).astype(BF)
    tail_a = jnp.where((shift == 8) & (c_slot < 4), 1.0, 0.0).astype(BF)
    tail_b = jnp.where((shift == 4) & (c_slot >= 4), 1.0, 0.0).astype(BF)

    def swap(block):
        return jnp.concatenate([block[4:], block[:4]], axis=0)

    def fill_rows(store, k, rows):
        for f in range(flight):
            top = rows[f * SLOTS:f * SLOTS + 8]
            bottom = rows[f * SLOTS + 8:(f + 1) * SLOTS]
            for d in range(n_d):
                at = d * cols
                store[k, d, f, :, :cols] = top[:, at:at + cols].astype(BF)
                store[k, d, f, :, cols:] = (
                    bottom[:, at:at + half] + swap(bottom[:, at + half:at + cols])
                ).astype(BF)

    def unpack(landing, k):
        flat = landing[k].reshape(group * 8, wide_cols)
        tail = flat[:, cols:]
        return jnp.concatenate(
            [
                mm(low_rows, flat[:, :half]) + mm(tail_a, tail),
                mm(low_rows, flat[:, half:cols]) + mm(tail_b, tail),
            ],
            axis=1,
        ).astype(BF)

    def spread(store, landing, k, phase):
        def one(ty, td):
            te = ty * CORES + core
            remote(
                store.at[k, td, te // SPLIT], landing.at[k, core, chip], k, phase, (sec, te, td)
            ).start()

        each(one)
        landing[k, core, chip] = store[k, dp, exp // SPLIT]

    def pass_on(landing, k, phase):
        wait_all(landing.at[k, 0, pl.ds(0, chips - 1)], k, phase)
        remote(landing.at[k, core], landing.at[k, core], k, phase + 1, sibling).start()

    def load_in(k):
        return inc[k]

    def tok_phase(k):
        rows = mm(picks[k][0], load_in(k))
        scale = lax.rsqrt(jnp.mean(rows * rows, axis=1, keepdims=True) + 0.5)
        fill_rows(toks, k, rows * scale * gain[...])

    for k in range(steps):
        sel, slot_gate = picks[k]
        if k == 0:
            loads[3].wait()
        tok_phase(k)
        if k == 0:
            pl.semaphore_wait(barrier, greeted)
        spread(toks, tokr, k, 0)
        if n_s > 1 and compact and k < steps - 1:
            place_s[k] = sel
            remote(place_s.at[k], place_r.at[k], k, 8, (nxt, exp, dp)).start()
            remote(inc.at[k], base.at[k], k, 9, (nxt, exp, dp)).start()
        if k == 0:
            loads[4].wait()
            for turn in range(steps):
                pick, share = picks[turn]
                fill_rows(cots, turn, mm(pick, cot[0, turn]) * share)
                spread(cots, cotr, turn, 2)

        pass_on(tokr, k, 0)
        wait_all(tokr.at[k, 0], k, 1)
        tok = unpack(tokr, k)
        if k == 0:
            for load in loads[5:]:
                load.wait()
        part_g = mm(tok, wg[0], 1, 1)
        part_u = mm(tok, wu[0], 1, 1)
        for d in range(n_d):
            parts[k, d, 0] = part_g[d * chunk:(d + 1) * chunk].astype(BF)
            parts[k, d, 1] = part_u[d * chunk:(d + 1) * chunk].astype(BF)
        for j in range(n_d - 1):
            td = lax.rem(dp + 1 + j, n_d)
            remote(parts.at[k, td], partr.at[k, dp], k, 4, (sec, exp, td)).start()
        partr[k, dp] = parts[k, dp]
        pass_on(cotr, k, 2)
        wait_all(partr.at[k, pl.ds(0, n_d - 1)], k, 4)
        act_g = sum(partr[k, d, 0].astype(F32) for d in range(n_d))
        act_u = sum(partr[k, d, 1].astype(F32) for d in range(n_d))
        hid[k, dp] = (act_g / (1.0 + jnp.exp(-act_g)) * act_u).astype(BF)
        for j in range(n_d - 1):
            td = far(j)
            remote(hid.at[k, dp], hid.at[k, dp], k, 5, (sec, exp, td)).start()
        wait_all(hid.at[k, pl.ds(0, n_d - 1)], k, 5)
        hidden = hid[k].reshape(n_d * chunk, wg.shape[1])
        piece = mm(hidden, wd[0]).astype(BF)
        rets[k, :, :, :, :cols] = mm(low_rows, piece, 0, 0).astype(BF).reshape(
            CORES, chips, 8, cols
        )
        rets[k, :, :, :, cols:] = (
            mm(tail_a, piece[:, :half], 0, 0) + mm(tail_b, piece[:, half:], 0, 0)
        ).astype(BF).reshape(CORES, chips, 8, half)

        remote(rets.at[k, 1 - core], pair.at[k], k, 6, sibling).start()
        wait_all(pair.at[k], k, 6)
        rsum[k] = (rets[k, core].astype(F32) + pair[k].astype(F32)).astype(BF)

        def give_back(ty, td):
            remote(
                rsum.at[k, ty * n_d + td], retr.at[k, mine_y, dp], k, 7,
                (sec, ty * CORES + core, td),
            ).start()

        each(give_back)
        retr[k, exp // CORES, dp] = rsum[k, chip]
        wait_all(cotr.at[k, 0], k, 3)
        part = mm(hidden, unpack(cotr, k), 0, 0)
        grad[0] = part if k == 0 else grad[0] + part

        wait_all(rsum.at[k, pl.ds(0, chips - 1)], k, 7)
        tops = []
        row_8 = lax.broadcasted_iota(jnp.int32, (8, half), 0)
        pairs = SPLIT // CORES
        for f in range(flight):
            top, tail = [], []
            for d in range(n_d):
                total = sum(retr[k, f * pairs + j, d].astype(F32) for j in range(pairs))
                top.append(total[:, :cols])
                last = total[:, cols:]
                tail.append(jnp.where(row_8 < 4, last, 0.0))
                tail.append(jnp.where(row_8 < 4, swap(last), 0.0))
            tops.append(jnp.concatenate(top, axis=1))
            tops.append(jnp.concatenate(tail, axis=1))
        mixed = jnp.concatenate(tops, axis=0) * slot_gate
        high = mixed.astype(BF)
        low = (mixed - high.astype(F32)).astype(BF)
        mixture = mm(sel, high, 0, 0) + mm(sel, low, 0, 0)
        result = (load_in(k).astype(F32) + mixture).astype(BF)
        out[0, k] = result
        if k + 1 < steps:
            if n_s == 1:
                inc[k + 1] = fresh[k]
            elif compact:
                rows_s[k] = mm(sel, result).astype(BF)
                remote(rows_s.at[k], rows_r.at[k], k, 10, (nxt, exp, dp)).start()
                wait_all(base.at[k], k, 9)
                wait_all(place_r.at[k], k, 8)
                wait_all(rows_r.at[k], k, 10)
                spot = place_r[k]
                if flight > 1:
                    u_row = lax.broadcasted_iota(jnp.int32, (used, used), 0) >> 4
                    u_col = lax.broadcasted_iota(jnp.int32, (used, used), 1) >> 4
                    sooner = jnp.where(u_col < u_row, 1.0, 0.0).astype(BF)
                    spot = jnp.where(mm(sooner, spot) > 0.5, 0.0, spot.astype(F32)).astype(BF)
                kept = mm(spot, jnp.ones((used, width), BF), 0, 0)
                moved = jnp.where(kept > 0.5, mm(spot, rows_r[k], 0, 0), base[k].astype(F32))
                inc[k + 1] = jnp.where(sec == 0, fresh[k].astype(F32), moved).astype(BF)
            else:
                remote(out.at[0, k], base.at[k], k, 9, (nxt, exp, dp)).start()
                wait_all(base.at[k], k, 9)
                inc[k + 1] = jnp.where(
                    sec == 0, fresh[k].astype(F32), base[k].astype(F32)
                ).astype(BF)

    for k in range(steps):
        wait_all(tokr.at[k, 0, pl.ds(0, chips - 1)], k, 0, True)
        wait_all(tokr.at[k, 0], k, 1, True)
        wait_all(cotr.at[k, 0, pl.ds(0, chips - 1)], k, 2, True)
        wait_all(cotr.at[k, 0], k, 3, True)
        wait_all(parts.at[k, pl.ds(0, n_d - 1)], k, 4, True)
        wait_all(hid.at[k, pl.ds(0, n_d - 1)], k, 5, True)
        wait_all(pair.at[k], k, 6, True)
        wait_all(rsum.at[k, pl.ds(0, chips - 1)], k, 7, True)
        if n_s > 1 and k < steps - 1:
            wait_all(base.at[k], k, 9, True)
            if compact:
                wait_all(place_s.at[k], k, 8, True)
                wait_all(rows_s.at[k], k, 10, True)


def local(sizes, arrivals, fresh, routes, gates, cotangent, norm_gain, w_gate, w_up, w_down):
    n_s, n_e, n_d = sizes
    steps = routes.shape[1]
    tok_rows, width = arrivals.shape[1:]
    units, cols = w_gate.shape[1:]
    flight = n_e // SPLIT
    chips = n_e * n_d // CORES
    chunk = CAP * n_e
    used = flight * SLOTS
    hops = max(steps - 1, 1)
    packed = cols + cols // 2
    vmem = pl.BlockSpec(memory_space=pltpu.VMEM)
    return pl.pallas_call(
        functools.partial(kernel, n_s, n_e, n_d, steps),
        out_shape=(
            jax.ShapeDtypeStruct((1, steps, tok_rows, width), BF),
            jax.ShapeDtypeStruct((1, units, cols), F32),
        ),
        in_specs=[pl.BlockSpec(memory_space=pltpu.HBM)] * 9,
        out_specs=(vmem, vmem),
        scratch_shapes=[
            pltpu.VMEM(fresh.shape, BF),
            pltpu.VMEM((1, routes.shape[3], steps, tok_rows), jnp.int32),
            pltpu.VMEM((1, routes.shape[3], steps, tok_rows), BF),
            pltpu.VMEM(cotangent.shape, BF),
            pltpu.VMEM(norm_gain.shape, F32),
            pltpu.VMEM(w_gate.shape, BF),
            pltpu.VMEM(w_up.shape, BF),
            pltpu.VMEM(w_down.shape, BF),
            pltpu.SemaphoreType.DMA((9,)),
            pltpu.VMEM((steps, n_d, flight, 8, packed), BF),
            pltpu.VMEM((steps, CORES, chips, 8, packed), BF),
            pltpu.VMEM((steps, n_d, flight, 8, packed), BF),
            pltpu.VMEM((steps, CORES, chips, 8, packed), BF),
            pltpu.VMEM((steps, n_d, 2, chunk, units), BF),
            pltpu.VMEM((steps, n_d, 2, chunk, units), BF),
            pltpu.VMEM((steps, n_d, chunk, units), BF),
            pltpu.VMEM((steps, CORES, chips, 8, packed), BF),
            pltpu.VMEM((steps, chips, 8, packed), BF),
            pltpu.VMEM((steps, chips, 8, packed), BF),
            pltpu.VMEM((steps, n_e // CORES, n_d, 8, packed), BF),
            pltpu.VMEM((hops, tok_rows, width), BF),
            pltpu.VMEM((steps, tok_rows, width), BF),
            pltpu.VMEM((hops, used, tok_rows), BF),
            pltpu.VMEM((hops, used, tok_rows), BF),
            pltpu.VMEM((hops, used, width), BF),
            pltpu.VMEM((hops, used, width), BF),
            pltpu.SemaphoreType.DMA((steps, 11)),
            pltpu.SemaphoreType.DMA((steps, 11)),
        ],
        compiler_params=pltpu.CompilerParams(
            collective_id=0, has_side_effects=True, vmem_limit_bytes=60000 * 1024
        ),
    )(
        arrivals, fresh, jnp.transpose(routes, (0, 3, 1, 2)),
        jnp.transpose(gates, (0, 3, 1, 2)), cotangent,
        norm_gain, w_gate, w_up, w_down,
    )


def solution(mesh):
    placed = (
        P("section", ("expert", "dp"), None),
        P(None, ("expert", "dp"), None),
        P("section", None, ("expert", "dp"), None),
        P("section", None, ("expert", "dp"), None),
        P("section", None, ("expert", "dp"), None),
        P("section", None),
        P("section", "expert", "dp"),
        P("section", "expert", "dp"),
        P("section", "expert", "dp"),
    )
    sizes = (mesh.shape["section"], mesh.shape["expert"], mesh.shape["dp"])
    return jax.shard_map(
        functools.partial(local, sizes),
        mesh=mesh,
        in_specs=placed,
        out_specs=(P("section", None, ("expert", "dp"), None), P("section", "expert", "dp")),
        check_vma=False,
    )
```

```python
import functools

import jax
import jax.numpy as jnp
from jax import lax
from jax.experimental import pallas as pl
from jax.experimental.pallas import tpu as pltpu
from jax.sharding import PartitionSpec as P

SPLIT = 4
CAP = 12
SLOTS = 16
CORES = 2
MESH = pl.DeviceIdType.MESH
BF = jnp.bfloat16
F32 = jnp.float32


def mm(a, b, ca=1, cb=0):
    return lax.dot_general(a, b, (((ca,), (cb,)), ((), ())), preferred_element_type=F32)


def kernel(
    n_s, n_e, n_d, steps,
    arr_h, fresh_h, routes_h, gates_h, cot_h, gain_h, wg_h, wu_h, wd_h,
    out, grad,
    fresh, routes, gates, cot, gain, wg, wu, wd, load_sems,
    toks, tokr, cots, cotr, parts, partr, hid, rets, pair, rsum, retr,
    base, inc, place_s, place_r, rows_s, rows_r,
    send_sems, recv_sems,
):
    sec = lax.axis_index("section")
    exp = lax.axis_index("expert")
    dp = lax.axis_index("dp")
    chips = n_e * n_d // CORES
    group = CORES * chips
    flight = n_e // SPLIT
    tok_rows, width = inc.shape[1:]
    cols = width // n_d
    half = cols // 2
    wide_cols = cols + half
    chunk = CAP * chips // n_d
    rows_half = CAP * chips
    used = flight * SLOTS
    compact = used < tok_rows
    core = lax.rem(exp, CORES)
    chip = (exp // CORES) * n_d + dp
    sibling = (sec, exp + 1 - 2 * core, dp)
    nxt = lax.rem(sec + 1, n_s)

    def far(j):
        low = n_d - 1 - j - (dp + j) // max(n_d - 1, 1)
        high = j + (j - dp + n_d) // n_d
        up = dp // ((n_d + 1) // 2)
        return up * high + (1 - up) * low

    n_y = n_e // CORES
    mine_y = exp // CORES

    def each(body):
        def far_one(i):
            body((mine_y + 1 + lax.rem(i, n_y)) % n_y, far(i // n_y))

        if chips <= 32:
            for i in range((n_d - 1) * n_y):
                body((mine_y + 1 + i % n_y) % n_y, far(i // n_y))
        else:
            @pl.loop(0, (n_d - 1) * n_y)
            def _(i):
                far_one(i)
        for o in range(1, n_y):
            body((mine_y + o) % n_y, dp)

    barrier = pltpu.get_barrier_semaphore()

    def signal(target):
        pl.semaphore_signal(barrier, inc=1, device_id=target, device_id_type=MESH)

    each(lambda ty, td: signal((sec, ty * CORES + core, td)))
    signal(sibling)
    greeted = chips
    for off in sorted({off for off in (1 % n_s, (n_s - 1) % n_s) if off}):
        signal((lax.rem(sec + off, n_s), exp, dp))
        greeted += 1

    loads = [
        pltpu.make_async_copy(src, dst, load_sems.at[i])
        for i, (src, dst) in enumerate((
            (routes_h, routes), (gates_h, gates), (gain_h, gain), (arr_h.at[0], inc.at[0]),
            (cot_h, cot), (wg_h, wg), (wu_h, wu), (wd_h, wd), (fresh_h, fresh),
        ))
    ]
    for load in loads:
        load.start()

    def remote(src, dst, k, phase, target):
        return pltpu.make_async_remote_copy(
            src_ref=src, dst_ref=dst, send_sem=send_sems.at[k, phase],
            recv_sem=recv_sems.at[k, phase], device_id=target, device_id_type=MESH,
        )

    def wait_all(ref, k, phase, send=False):
        copy = remote(ref, ref, k, phase, sibling)
        if send:
            copy.wait_send()
        else:
            copy.wait_recv()

    for load in loads[:3]:
        load.wait()

    lane = lax.broadcasted_iota(jnp.int32, (used, tok_rows), 0)
    lane_expert = lane >> 4
    lane_slot = lane & (SLOTS - 1)
    t_row = lax.broadcasted_iota(jnp.int32, (tok_rows, tok_rows), 0)
    t_col = lax.broadcasted_iota(jnp.int32, (tok_rows, tok_rows), 1)
    earlier_tok = jnp.where(t_row < t_col, 1.0, 0.0).astype(BF)

    def selection(k):
        naming = jnp.zeros((used, tok_rows), F32)
        shares = jnp.zeros((used, tok_rows), F32)
        for j in range(routes.shape[1]):
            hit = routes[0, j, k:k + 1, :] == lane_expert
            naming = jnp.where(hit, 1.0, naming)
            shares = shares + jnp.where(hit, gates[0, j].astype(F32)[k:k + 1, :], 0.0)
        places = mm(naming.astype(BF), earlier_tok)
        chosen = jnp.where(places == lane_slot.astype(F32), naming, 0.0)
        chosen = jnp.where(lane_slot < CAP, chosen, 0.0)
        slot_gate = jnp.sum(chosen * shares, axis=1, keepdims=True)
        return chosen.astype(BF), slot_gate

    picks = [selection(k) for k in range(steps)]

    r_i = lax.broadcasted_iota(jnp.int32, (CAP * chips, 8 * chips), 0)
    c_i = lax.broadcasted_iota(jnp.int32, (CAP * chips, 8 * chips), 1)
    c_slot = c_i & 7
    shift = r_i - (c_i >> 3) * CAP - c_slot
    low_rows = jnp.where(shift == 0, 1.0, 0.0).astype(BF)
    tail_a = jnp.where((shift == 8) & (c_slot < 4), 1.0, 0.0).astype(BF)
    tail_b = jnp.where((shift == 4) & (c_slot >= 4), 1.0, 0.0).astype(BF)

    def swap(block):
        return jnp.concatenate([block[4:], block[:4]], axis=0)

    def fill_rows(store, k, rows):
        for f in range(flight):
            top = rows[f * SLOTS:f * SLOTS + 8]
            bottom = rows[f * SLOTS + 8:(f + 1) * SLOTS]
            for d in range(n_d):
                at = d * cols
                store[k, d, f, :, :cols] = top[:, at:at + cols].astype(BF)
                store[k, d, f, :, cols:] = (
                    bottom[:, at:at + half] + swap(bottom[:, at + half:at + cols])
                ).astype(BF)

    def unpack(landing, k, part):
        flat = landing[k, part].reshape(chips * 8, wide_cols)
        tail = flat[:, cols:]
        return jnp.concatenate(
            [
                mm(low_rows, flat[:, :half]) + mm(tail_a, tail),
                mm(low_rows, flat[:, half:cols]) + mm(tail_b, tail),
            ],
            axis=1,
        ).astype(BF)

    def spread(store, landing, k, phase):
        def one(ty, td):
            te = ty * CORES + core
            remote(
                store.at[k, td, te // SPLIT], landing.at[k, core, chip], k, phase, (sec, te, td)
            ).start()

        each(one)
        landing[k, core, chip] = store[k, dp, exp // SPLIT]

    def pass_on(landing, k, phase):
        wait_all(landing.at[k, 0, pl.ds(0, chips - 1)], k, phase)
        remote(landing.at[k, core], landing.at[k, core], k, phase + 1, sibling).start()

    def load_in(k):
        return inc[k]

    def tok_phase(k):
        rows = mm(picks[k][0], load_in(k))
        scale = lax.rsqrt(jnp.mean(rows * rows, axis=1, keepdims=True) + 0.5)
        fill_rows(toks, k, rows * scale * gain[...])

    for k in range(steps):
        sel, slot_gate = picks[k]
        if k == 0:
            loads[3].wait()
        tok_phase(k)
        if k == 0:
            pl.semaphore_wait(barrier, greeted)
        spread(toks, tokr, k, 0)
        if n_s > 1 and compact and k < steps - 1:
            place_s[k] = sel
            remote(place_s.at[k], place_r.at[k], k, 8, (nxt, exp, dp)).start()
            remote(inc.at[k], base.at[k], k, 9, (nxt, exp, dp)).start()
        if k == 0:
            loads[4].wait()
            for turn in range(steps):
                pick, share = picks[turn]
                fill_rows(cots, turn, mm(pick, cot[0, turn]) * share)
                spread(cots, cotr, turn, 2)

        pass_on(tokr, k, 0)
        if k == 0:
            for load in loads[5:]:
                load.wait()

        def partial_sums(part, phase):
            tok = unpack(tokr, k, part)
            for i, weight in enumerate((wg, wu)):
                acted = mm(tok, weight[0], 1, 1)
                for d in range(n_d):
                    parts[k, part, d, i] = acted[d * chunk:(d + 1) * chunk].astype(BF)
            for j in range(n_d - 1):
                td = lax.rem(dp + 1 + j, n_d)
                remote(
                    parts.at[k, part, td], partr.at[k, part, dp], k, phase, (sec, exp, td)
                ).start()
            partr[k, part, dp] = parts[k, part, dp]

        def activate(part, phase):
            wait_all(partr.at[k, 0, pl.ds(0, n_d - 1)], k, phase)
            act_g = sum(partr[k, part, d, 0].astype(F32) for d in range(n_d))
            act_u = sum(partr[k, part, d, 1].astype(F32) for d in range(n_d))
            hid[k, part, dp] = (act_g / (1.0 + jnp.exp(-act_g)) * act_u).astype(BF)
            for j in range(n_d - 1):
                mine = hid.at[k, part, dp]
                remote(mine, mine, k, phase + 1, (sec, exp, far(j))).start()

        def down(part, phase):
            wait_all(hid.at[k, 0, pl.ds(0, n_d - 1)], k, phase + 1)
            hidden = hid[k, part].reshape(rows_half, wg.shape[1])
            piece = mm(hidden, wd[0]).astype(BF)
            rets[k, part, :, :, :cols] = mm(low_rows, piece, 0, 0).astype(BF).reshape(
                chips, 8, cols
            )
            rets[k, part, :, :, cols:] = (
                mm(tail_a, piece[:, :half], 0, 0) + mm(tail_b, piece[:, half:], 0, 0)
            ).astype(BF).reshape(chips, 8, half)

        partial_sums(core, 4)
        wait_all(tokr.at[k, 0], k, 1)
        partial_sums(1 - core, 11)
        pass_on(cotr, k, 2)
        activate(core, 4)
        activate(1 - core, 11)
        down(core, 4)
        down(1 - core, 11)

        remote(rets.at[k, 1 - core], pair.at[k], k, 6, sibling).start()
        wait_all(pair.at[k], k, 6)
        rsum[k] = (rets[k, core].astype(F32) + pair[k].astype(F32)).astype(BF)

        def give_back(ty, td):
            remote(
                rsum.at[k, ty * n_d + td], retr.at[k, mine_y, dp], k, 7,
                (sec, ty * CORES + core, td),
            ).start()

        each(give_back)
        retr[k, exp // CORES, dp] = rsum[k, chip]
        wait_all(cotr.at[k, 0], k, 3)
        part = sum(
            mm(hid[k, c].reshape(rows_half, wg.shape[1]), unpack(cotr, k, c), 0, 0)
            for c in range(CORES)
        )
        grad[0] = part if k == 0 else grad[0] + part

        wait_all(rsum.at[k, pl.ds(0, chips - 1)], k, 7)
        tops = []
        row_8 = lax.broadcasted_iota(jnp.int32, (8, half), 0)
        pairs = SPLIT // CORES
        for f in range(flight):
            top, tail = [], []
            for d in range(n_d):
                total = sum(retr[k, f * pairs + j, d].astype(F32) for j in range(pairs))
                top.append(total[:, :cols])
                last = total[:, cols:]
                tail.append(jnp.where(row_8 < 4, last, 0.0))
                tail.append(jnp.where(row_8 < 4, swap(last), 0.0))
            tops.append(jnp.concatenate(top, axis=1))
            tops.append(jnp.concatenate(tail, axis=1))
        mixed = jnp.concatenate(tops, axis=0) * slot_gate
        high = mixed.astype(BF)
        low = (mixed - high.astype(F32)).astype(BF)
        mixture = mm(sel, high, 0, 0) + mm(sel, low, 0, 0)
        result = (load_in(k).astype(F32) + mixture).astype(BF)
        out[0, k] = result
        if k + 1 < steps:
            if n_s == 1:
                inc[k + 1] = fresh[k]
            elif compact:
                rows_s[k] = mm(sel, result).astype(BF)
                remote(rows_s.at[k], rows_r.at[k], k, 10, (nxt, exp, dp)).start()
                wait_all(base.at[k], k, 9)
                wait_all(place_r.at[k], k, 8)
                wait_all(rows_r.at[k], k, 10)
                spot = place_r[k]
                if flight > 1:
                    u_row = lax.broadcasted_iota(jnp.int32, (used, used), 0) >> 4
                    u_col = lax.broadcasted_iota(jnp.int32, (used, used), 1) >> 4
                    sooner = jnp.where(u_col < u_row, 1.0, 0.0).astype(BF)
                    spot = jnp.where(mm(sooner, spot) > 0.5, 0.0, spot.astype(F32)).astype(BF)
                kept = mm(spot, jnp.ones((used, width), BF), 0, 0)
                moved = jnp.where(kept > 0.5, mm(spot, rows_r[k], 0, 0), base[k].astype(F32))
                inc[k + 1] = jnp.where(sec == 0, fresh[k].astype(F32), moved).astype(BF)
            else:
                remote(out.at[0, k], base.at[k], k, 9, (nxt, exp, dp)).start()
                wait_all(base.at[k], k, 9)
                inc[k + 1] = jnp.where(
                    sec == 0, fresh[k].astype(F32), base[k].astype(F32)
                ).astype(BF)

    for k in range(steps):
        wait_all(tokr.at[k, 0, pl.ds(0, chips - 1)], k, 0, True)
        wait_all(tokr.at[k, 0], k, 1, True)
        wait_all(cotr.at[k, 0, pl.ds(0, chips - 1)], k, 2, True)
        wait_all(cotr.at[k, 0], k, 3, True)
        for phase in (4, 11):
            wait_all(parts.at[k, 0, pl.ds(0, n_d - 1)], k, phase, True)
            wait_all(hid.at[k, 0, pl.ds(0, n_d - 1)], k, phase + 1, True)
        wait_all(pair.at[k], k, 6, True)
        wait_all(rsum.at[k, pl.ds(0, chips - 1)], k, 7, True)
        if n_s > 1 and k < steps - 1:
            wait_all(base.at[k], k, 9, True)
            if compact:
                wait_all(place_s.at[k], k, 8, True)
                wait_all(rows_s.at[k], k, 10, True)


def local(sizes, arrivals, fresh, routes, gates, cotangent, norm_gain, w_gate, w_up, w_down):
    n_s, n_e, n_d = sizes
    steps = routes.shape[1]
    tok_rows, width = arrivals.shape[1:]
    units, cols = w_gate.shape[1:]
    flight = n_e // SPLIT
    chips = n_e * n_d // CORES
    chunk = CAP * chips // n_d
    used = flight * SLOTS
    hops = max(steps - 1, 1)
    packed = cols + cols // 2
    vmem = pl.BlockSpec(memory_space=pltpu.VMEM)
    return pl.pallas_call(
        functools.partial(kernel, n_s, n_e, n_d, steps),
        out_shape=(
            jax.ShapeDtypeStruct((1, steps, tok_rows, width), BF),
            jax.ShapeDtypeStruct((1, units, cols), F32),
        ),
        in_specs=[pl.BlockSpec(memory_space=pltpu.HBM)] * 9,
        out_specs=(vmem, vmem),
        scratch_shapes=[
            pltpu.VMEM(fresh.shape, BF),
            pltpu.VMEM((1, routes.shape[3], steps, tok_rows), jnp.int32),
            pltpu.VMEM((1, routes.shape[3], steps, tok_rows), BF),
            pltpu.VMEM(cotangent.shape, BF),
            pltpu.VMEM(norm_gain.shape, F32),
            pltpu.VMEM(w_gate.shape, BF),
            pltpu.VMEM(w_up.shape, BF),
            pltpu.VMEM(w_down.shape, BF),
            pltpu.SemaphoreType.DMA((9,)),
            pltpu.VMEM((steps, n_d, flight, 8, packed), BF),
            pltpu.VMEM((steps, CORES, chips, 8, packed), BF),
            pltpu.VMEM((steps, n_d, flight, 8, packed), BF),
            pltpu.VMEM((steps, CORES, chips, 8, packed), BF),
            pltpu.VMEM((steps, CORES, n_d, 2, chunk, units), BF),
            pltpu.VMEM((steps, CORES, n_d, 2, chunk, units), BF),
            pltpu.VMEM((steps, CORES, n_d, chunk, units), BF),
            pltpu.VMEM((steps, CORES, chips, 8, packed), BF),
            pltpu.VMEM((steps, chips, 8, packed), BF),
            pltpu.VMEM((steps, chips, 8, packed), BF),
            pltpu.VMEM((steps, n_e // CORES, n_d, 8, packed), BF),
            pltpu.VMEM((hops, tok_rows, width), BF),
            pltpu.VMEM((steps, tok_rows, width), BF),
            pltpu.VMEM((hops, used, tok_rows), BF),
            pltpu.VMEM((hops, used, tok_rows), BF),
            pltpu.VMEM((hops, used, width), BF),
            pltpu.VMEM((hops, used, width), BF),
            pltpu.SemaphoreType.DMA((steps, 13)),
            pltpu.SemaphoreType.DMA((steps, 13)),
        ],
        compiler_params=pltpu.CompilerParams(
            collective_id=0, has_side_effects=True, vmem_limit_bytes=60000 * 1024
        ),
    )(
        arrivals, fresh, jnp.transpose(routes, (0, 3, 1, 2)),
        jnp.transpose(gates, (0, 3, 1, 2)), cotangent,
        norm_gain, w_gate, w_up, w_down,
    )


def solution(mesh):
    placed = (
        P("section", ("expert", "dp"), None),
        P(None, ("expert", "dp"), None),
        P("section", None, ("expert", "dp"), None),
        P("section", None, ("expert", "dp"), None),
        P("section", None, ("expert", "dp"), None),
        P("section", None),
        P("section", "expert", "dp"),
        P("section", "expert", "dp"),
        P("section", "expert", "dp"),
    )
    sizes = (mesh.shape["section"], mesh.shape["expert"], mesh.shape["dp"])
    return jax.shard_map(
        functools.partial(local, sizes),
        mesh=mesh,
        in_specs=placed,
        out_specs=(P("section", None, ("expert", "dp"), None), P("section", "expert", "dp")),
        check_vma=False,
    )
```

```python
import functools

import jax
import jax.numpy as jnp
from jax import lax
from jax.experimental import pallas as pl
from jax.experimental.pallas import tpu as pltpu
from jax.sharding import PartitionSpec as P

SPLIT = 4
CAP = 12
SLOTS = 16
CORES = 2
MESH = pl.DeviceIdType.MESH
BF = jnp.bfloat16
F32 = jnp.float32


def mm(a, b, ca=1, cb=0):
    return lax.dot_general(a, b, (((ca,), (cb,)), ((), ())), preferred_element_type=F32)


def kernel(
    n_s, n_e, n_d, steps,
    arr_h, fresh_h, routes_h, gates_h, cot_h, gain_h, wg_h, wu_h, wd_h,
    out, grad,
    out_v, grad_v, store_sems, fresh, routes, gates, cot, gain, wg, wu, wd, load_sems,
    toks, tokr, cots, cotr, parts, partr, hid, rets, pair, rsum, retr,
    base, inc, place_s, place_r, rows_s, rows_r,
    send_sems, recv_sems,
):
    sec = lax.axis_index("section")
    exp = lax.axis_index("expert")
    dp = lax.axis_index("dp")
    chips = n_e * n_d // CORES
    group = CORES * chips
    flight = n_e // SPLIT
    tok_rows, width = inc.shape[1:]
    cols = width // n_d
    half = cols // 2
    wide_cols = cols + half
    chunk = CAP * chips // n_d
    rows_half = CAP * chips
    used = flight * SLOTS
    compact = used < tok_rows
    core = lax.rem(exp, CORES)
    chip = (exp // CORES) * n_d + dp
    sibling = (sec, exp + 1 - 2 * core, dp)
    nxt = lax.rem(sec + 1, n_s)

    def far(j):
        low = n_d - 1 - j - (dp + j) // max(n_d - 1, 1)
        high = j + (j - dp + n_d) // n_d
        up = dp // ((n_d + 1) // 2)
        return up * high + (1 - up) * low

    n_y = n_e // CORES
    mine_y = exp // CORES

    def each(body):
        def far_one(i):
            body((mine_y + 1 + lax.rem(i, n_y)) % n_y, far(i // n_y))

        if chips <= 32:
            for i in range((n_d - 1) * n_y):
                body((mine_y + 1 + i % n_y) % n_y, far(i // n_y))
        else:
            @pl.loop(0, (n_d - 1) * n_y)
            def _(i):
                far_one(i)
        for o in range(1, n_y):
            body((mine_y + o) % n_y, dp)

    barrier = pltpu.get_barrier_semaphore()

    def signal(target):
        pl.semaphore_signal(barrier, inc=1, device_id=target, device_id_type=MESH)

    each(lambda ty, td: signal((sec, ty * CORES + core, td)))
    signal(sibling)
    greeted = chips
    for off in sorted({off for off in (1 % n_s, (n_s - 1) % n_s) if off}):
        signal((lax.rem(sec + off, n_s), exp, dp))
        greeted += 1

    loads = [
        pltpu.make_async_copy(src, dst, load_sems.at[i])
        for i, (src, dst) in enumerate((
            (routes_h, routes), (gates_h, gates), (gain_h, gain), (arr_h.at[0], inc.at[0]),
            (cot_h, cot), (wg_h, wg), (wu_h, wu), (wd_h, wd), (fresh_h, fresh),
        ))
    ]
    for load in loads:
        load.start()

    def remote(src, dst, k, phase, target):
        return pltpu.make_async_remote_copy(
            src_ref=src, dst_ref=dst, send_sem=send_sems.at[k, phase],
            recv_sem=recv_sems.at[k, phase], device_id=target, device_id_type=MESH,
        )

    def wait_all(ref, k, phase, send=False):
        copy = remote(ref, ref, k, phase, sibling)
        if send:
            copy.wait_send()
        else:
            copy.wait_recv()

    for load in loads[:3]:
        load.wait()

    lane = lax.broadcasted_iota(jnp.int32, (used, tok_rows), 0)
    lane_expert = lane >> 4
    lane_slot = lane & (SLOTS - 1)
    t_row = lax.broadcasted_iota(jnp.int32, (tok_rows, tok_rows), 0)
    t_col = lax.broadcasted_iota(jnp.int32, (tok_rows, tok_rows), 1)
    earlier_tok = jnp.where(t_row < t_col, 1.0, 0.0).astype(BF)

    def selection(k):
        naming = jnp.zeros((used, tok_rows), F32)
        shares = jnp.zeros((used, tok_rows), F32)
        for j in range(routes.shape[1]):
            hit = routes[0, j, k:k + 1, :] == lane_expert
            naming = jnp.where(hit, 1.0, naming)
            shares = shares + jnp.where(hit, gates[0, j].astype(F32)[k:k + 1, :], 0.0)
        places = mm(naming.astype(BF), earlier_tok)
        chosen = jnp.where(places == lane_slot.astype(F32), naming, 0.0)
        chosen = jnp.where(lane_slot < CAP, chosen, 0.0)
        slot_gate = jnp.sum(chosen * shares, axis=1, keepdims=True)
        return chosen.astype(BF), slot_gate

    picks = [selection(k) for k in range(steps)]

    r_i = lax.broadcasted_iota(jnp.int32, (CAP * chips, 8 * chips), 0)
    c_i = lax.broadcasted_iota(jnp.int32, (CAP * chips, 8 * chips), 1)
    c_slot = c_i & 7
    shift = r_i - (c_i >> 3) * CAP - c_slot
    low_rows = jnp.where(shift == 0, 1.0, 0.0).astype(BF)
    tail_a = jnp.where((shift == 8) & (c_slot < 4), 1.0, 0.0).astype(BF)
    tail_b = jnp.where((shift == 4) & (c_slot >= 4), 1.0, 0.0).astype(BF)

    def swap(block):
        return jnp.concatenate([block[4:], block[:4]], axis=0)

    def fill_rows(store, k, rows):
        for f in range(flight):
            top = rows[f * SLOTS:f * SLOTS + 8]
            bottom = rows[f * SLOTS + 8:(f + 1) * SLOTS]
            for d in range(n_d):
                at = d * cols
                store[k, d, f, :, :cols] = top[:, at:at + cols].astype(BF)
                store[k, d, f, :, cols:] = (
                    bottom[:, at:at + half] + swap(bottom[:, at + half:at + cols])
                ).astype(BF)

    def unpack(landing, k, part):
        flat = landing[k, part].reshape(chips * 8, wide_cols)
        tail = flat[:, cols:]
        return jnp.concatenate(
            [
                mm(low_rows, flat[:, :half]) + mm(tail_a, tail),
                mm(low_rows, flat[:, half:cols]) + mm(tail_b, tail),
            ],
            axis=1,
        ).astype(BF)

    def spread(store, landing, k, phase):
        def one(ty, td):
            te = ty * CORES + core
            remote(
                store.at[k, td, te // SPLIT], landing.at[k, core, chip], k, phase, (sec, te, td)
            ).start()

        each(one)
        landing[k, core, chip] = store[k, dp, exp // SPLIT]

    def pass_on(landing, k, phase):
        wait_all(landing.at[k, 0, pl.ds(0, chips - 1)], k, phase)
        remote(landing.at[k, core], landing.at[k, core], k, phase + 1, sibling).start()

    def load_in(k):
        return inc[k]

    def tok_phase(k):
        rows = mm(picks[k][0], load_in(k))
        scale = lax.rsqrt(jnp.mean(rows * rows, axis=1, keepdims=True) + 0.5)
        fill_rows(toks, k, rows * scale * gain[...])

    for k in range(steps):
        sel, slot_gate = picks[k]
        if k == 0:
            loads[3].wait()
        tok_phase(k)
        if k == 0:
            pl.semaphore_wait(barrier, greeted)
        spread(toks, tokr, k, 0)
        if n_s > 1 and compact and k < steps - 1:
            place_s[k] = sel
            remote(place_s.at[k], place_r.at[k], k, 8, (nxt, exp, dp)).start()
            remote(inc.at[k], base.at[k], k, 9, (nxt, exp, dp)).start()
        if k == 0:
            loads[4].wait()
            for turn in range(steps):
                pick, share = picks[turn]
                fill_rows(cots, turn, mm(pick, cot[0, turn]) * share)
                spread(cots, cotr, turn, 2)

        pass_on(tokr, k, 0)
        if k == 0:
            for load in loads[5:]:
                load.wait()

        def partial_sums(part, phase):
            tok = unpack(tokr, k, part)
            for i, weight in enumerate((wg, wu)):
                acted = mm(tok, weight[0], 1, 1)
                for d in range(n_d):
                    parts[k, part, d, i] = acted[d * chunk:(d + 1) * chunk].astype(BF)
            for j in range(n_d - 1):
                td = lax.rem(dp + 1 + j, n_d)
                remote(
                    parts.at[k, part, td], partr.at[k, part, dp], k, phase, (sec, exp, td)
                ).start()
            partr[k, part, dp] = parts[k, part, dp]

        def activate(part, phase):
            wait_all(partr.at[k, 0, pl.ds(0, n_d - 1)], k, phase)
            act_g = sum(partr[k, part, d, 0].astype(F32) for d in range(n_d))
            act_u = sum(partr[k, part, d, 1].astype(F32) for d in range(n_d))
            hid[k, part, dp] = (act_g / (1.0 + jnp.exp(-act_g)) * act_u).astype(BF)
            for j in range(n_d - 1):
                mine = hid.at[k, part, dp]
                remote(mine, mine, k, phase + 1, (sec, exp, far(j))).start()

        def down(part, phase):
            wait_all(hid.at[k, 0, pl.ds(0, n_d - 1)], k, phase + 1)
            hidden = hid[k, part].reshape(rows_half, wg.shape[1])
            piece = mm(hidden, wd[0]).astype(BF)
            rets[k, part, :, :, :cols] = mm(low_rows, piece, 0, 0).astype(BF).reshape(
                chips, 8, cols
            )
            rets[k, part, :, :, cols:] = (
                mm(tail_a, piece[:, :half], 0, 0) + mm(tail_b, piece[:, half:], 0, 0)
            ).astype(BF).reshape(chips, 8, half)

        partial_sums(core, 4)
        wait_all(tokr.at[k, 0], k, 1)
        partial_sums(1 - core, 11)
        pass_on(cotr, k, 2)
        activate(core, 4)
        activate(1 - core, 11)
        down(core, 4)
        down(1 - core, 11)

        remote(rets.at[k, 1 - core], pair.at[k], k, 6, sibling).start()
        wait_all(pair.at[k], k, 6)
        rsum[k] = (rets[k, core].astype(F32) + pair[k].astype(F32)).astype(BF)

        def give_back(ty, td):
            remote(
                rsum.at[k, ty * n_d + td], retr.at[k, mine_y, dp], k, 7,
                (sec, ty * CORES + core, td),
            ).start()

        each(give_back)
        retr[k, exp // CORES, dp] = rsum[k, chip]
        wait_all(cotr.at[k, 0], k, 3)
        part = sum(
            mm(hid[k, c].reshape(rows_half, wg.shape[1]), unpack(cotr, k, c), 0, 0)
            for c in range(CORES)
        )
        grad_v[...] = part if k == 0 else grad_v[...] + part
        if k == steps - 1:
            pltpu.make_async_copy(grad_v, grad.at[0], store_sems.at[steps]).start()

        wait_all(rsum.at[k, pl.ds(0, chips - 1)], k, 7)
        tops = []
        row_8 = lax.broadcasted_iota(jnp.int32, (8, half), 0)
        pairs = SPLIT // CORES
        for f in range(flight):
            top, tail = [], []
            for d in range(n_d):
                total = sum(retr[k, f * pairs + j, d].astype(F32) for j in range(pairs))
                top.append(total[:, :cols])
                last = total[:, cols:]
                tail.append(jnp.where(row_8 < 4, last, 0.0))
                tail.append(jnp.where(row_8 < 4, swap(last), 0.0))
            tops.append(jnp.concatenate(top, axis=1))
            tops.append(jnp.concatenate(tail, axis=1))
        mixed = jnp.concatenate(tops, axis=0) * slot_gate
        high = mixed.astype(BF)
        low = (mixed - high.astype(F32)).astype(BF)
        mixture = mm(sel, high, 0, 0) + mm(sel, low, 0, 0)
        result = (load_in(k).astype(F32) + mixture).astype(BF)
        out_v[k] = result
        pltpu.make_async_copy(out_v.at[k], out.at[0, k], store_sems.at[k]).start()
        if k + 1 < steps:
            if n_s == 1:
                inc[k + 1] = fresh[k]
            elif compact:
                rows_s[k] = mm(sel, result).astype(BF)
                remote(rows_s.at[k], rows_r.at[k], k, 10, (nxt, exp, dp)).start()
                wait_all(base.at[k], k, 9)
                wait_all(place_r.at[k], k, 8)
                wait_all(rows_r.at[k], k, 10)
                spot = place_r[k]
                if flight > 1:
                    u_row = lax.broadcasted_iota(jnp.int32, (used, used), 0) >> 4
                    u_col = lax.broadcasted_iota(jnp.int32, (used, used), 1) >> 4
                    sooner = jnp.where(u_col < u_row, 1.0, 0.0).astype(BF)
                    spot = jnp.where(mm(sooner, spot) > 0.5, 0.0, spot.astype(F32)).astype(BF)
                kept = mm(spot, jnp.ones((used, width), BF), 0, 0)
                moved = jnp.where(kept > 0.5, mm(spot, rows_r[k], 0, 0), base[k].astype(F32))
                inc[k + 1] = jnp.where(sec == 0, fresh[k].astype(F32), moved).astype(BF)
            else:
                remote(out_v.at[k], base.at[k], k, 9, (nxt, exp, dp)).start()
                wait_all(base.at[k], k, 9)
                inc[k + 1] = jnp.where(
                    sec == 0, fresh[k].astype(F32), base[k].astype(F32)
                ).astype(BF)

    pltpu.make_async_copy(grad_v, grad.at[0], store_sems.at[steps]).wait()
    for k in range(steps):
        wait_all(tokr.at[k, 0, pl.ds(0, chips - 1)], k, 0, True)
        pltpu.make_async_copy(out_v.at[k], out.at[0, k], store_sems.at[k]).wait()
        wait_all(tokr.at[k, 0], k, 1, True)
        wait_all(cotr.at[k, 0, pl.ds(0, chips - 1)], k, 2, True)
        wait_all(cotr.at[k, 0], k, 3, True)
        for phase in (4, 11):
            wait_all(parts.at[k, 0, pl.ds(0, n_d - 1)], k, phase, True)
            wait_all(hid.at[k, 0, pl.ds(0, n_d - 1)], k, phase + 1, True)
        wait_all(pair.at[k], k, 6, True)
        wait_all(rsum.at[k, pl.ds(0, chips - 1)], k, 7, True)
        if n_s > 1 and k < steps - 1:
            wait_all(base.at[k], k, 9, True)
            if compact:
                wait_all(place_s.at[k], k, 8, True)
                wait_all(rows_s.at[k], k, 10, True)


def finish(out_in, grad_in, out, grad, out_v, grad_v, in_sems, out_sems):
    steps, tok_rows = out_v.shape[1:3]
    units = grad_v.shape[1]
    moves = []
    for k in range(steps):
        for h in range(2):
            part = (0, k, pl.ds(h * tok_rows // 2, tok_rows // 2))
            moves.append((out_in.at[part], out_v.at[part], out.at[part]))
    for h in range(4):
        part = (0, pl.ds(h * units // 4, units // 4))
        moves.append((grad_in.at[part], grad_v.at[part], grad.at[part]))
    loads = [
        pltpu.make_async_copy(src, held, in_sems.at[i]) for i, (src, held, _) in enumerate(moves)
    ]
    stores = [
        pltpu.make_async_copy(held, dst, out_sems.at[i]) for i, (_, held, dst) in enumerate(moves)
    ]
    for load in loads:
        load.start()
    for load, store in zip(loads, stores):
        load.wait()
        store.start()
    for store in stores:
        store.wait()


def local(sizes, arrivals, fresh, routes, gates, cotangent, norm_gain, w_gate, w_up, w_down):
    n_s, n_e, n_d = sizes
    steps = routes.shape[1]
    tok_rows, width = arrivals.shape[1:]
    units, cols = w_gate.shape[1:]
    flight = n_e // SPLIT
    chips = n_e * n_d // CORES
    chunk = CAP * chips // n_d
    used = flight * SLOTS
    hops = max(steps - 1, 1)
    packed = cols + cols // 2
    hbm = pl.BlockSpec(memory_space=pltpu.HBM)
    made = pl.pallas_call(
        functools.partial(kernel, n_s, n_e, n_d, steps),
        out_shape=(
            jax.ShapeDtypeStruct((1, steps, tok_rows, width), BF),
            jax.ShapeDtypeStruct((1, units, cols), F32),
        ),
        in_specs=[hbm] * 9,
        out_specs=(hbm, hbm),
        scratch_shapes=[
            pltpu.VMEM((steps, tok_rows, width), BF),
            pltpu.VMEM((units, cols), F32),
            pltpu.SemaphoreType.DMA((steps + 1,)),
            pltpu.VMEM(fresh.shape, BF),
            pltpu.VMEM((1, routes.shape[3], steps, tok_rows), jnp.int32),
            pltpu.VMEM((1, routes.shape[3], steps, tok_rows), BF),
            pltpu.VMEM(cotangent.shape, BF),
            pltpu.VMEM(norm_gain.shape, F32),
            pltpu.VMEM(w_gate.shape, BF),
            pltpu.VMEM(w_up.shape, BF),
            pltpu.VMEM(w_down.shape, BF),
            pltpu.SemaphoreType.DMA((9,)),
            pltpu.VMEM((steps, n_d, flight, 8, packed), BF),
            pltpu.VMEM((steps, CORES, chips, 8, packed), BF),
            pltpu.VMEM((steps, n_d, flight, 8, packed), BF),
            pltpu.VMEM((steps, CORES, chips, 8, packed), BF),
            pltpu.VMEM((steps, CORES, n_d, 2, chunk, units), BF),
            pltpu.VMEM((steps, CORES, n_d, 2, chunk, units), BF),
            pltpu.VMEM((steps, CORES, n_d, chunk, units), BF),
            pltpu.VMEM((steps, CORES, chips, 8, packed), BF),
            pltpu.VMEM((steps, chips, 8, packed), BF),
            pltpu.VMEM((steps, chips, 8, packed), BF),
            pltpu.VMEM((steps, n_e // CORES, n_d, 8, packed), BF),
            pltpu.VMEM((hops, tok_rows, width), BF),
            pltpu.VMEM((steps, tok_rows, width), BF),
            pltpu.VMEM((hops, used, tok_rows), BF),
            pltpu.VMEM((hops, used, tok_rows), BF),
            pltpu.VMEM((hops, used, width), BF),
            pltpu.VMEM((hops, used, width), BF),
            pltpu.SemaphoreType.DMA((steps, 13)),
            pltpu.SemaphoreType.DMA((steps, 13)),
        ],
        compiler_params=pltpu.CompilerParams(
            collective_id=0, has_side_effects=True, vmem_limit_bytes=60000 * 1024
        ),
    )(
        arrivals, fresh, jnp.transpose(routes, (0, 3, 1, 2)),
        jnp.transpose(gates, (0, 3, 1, 2)), cotangent,
        norm_gain, w_gate, w_up, w_down,
    )
    pieces = steps * 2 + 4
    return pl.pallas_call(
        finish,
        out_shape=tuple(jax.ShapeDtypeStruct(m.shape, m.dtype) for m in made),
        in_specs=[hbm] * 2,
        out_specs=(hbm, hbm),
        scratch_shapes=[pltpu.VMEM(m.shape, m.dtype) for m in made]
        + [pltpu.SemaphoreType.DMA((pieces,)), pltpu.SemaphoreType.DMA((pieces,))],
        compiler_params=pltpu.CompilerParams(vmem_limit_bytes=60000 * 1024),
    )(*made)


def solution(mesh):
    placed = (
        P("section", ("expert", "dp"), None),
        P(None, ("expert", "dp"), None),
        P("section", None, ("expert", "dp"), None),
        P("section", None, ("expert", "dp"), None),
        P("section", None, ("expert", "dp"), None),
        P("section", None),
        P("section", "expert", "dp"),
        P("section", "expert", "dp"),
        P("section", "expert", "dp"),
    )
    sizes = (mesh.shape["section"], mesh.shape["expert"], mesh.shape["dp"])
    return jax.shard_map(
        functools.partial(local, sizes),
        mesh=mesh,
        in_specs=placed,
        out_specs=(P("section", None, ("expert", "dp"), None), P("section", "expert", "dp")),
        check_vma=False,
    )
```

```python
import functools

import jax
import jax.numpy as jnp
from jax import lax
from jax.experimental import pallas as pl
from jax.experimental.pallas import tpu as pltpu
from jax.sharding import PartitionSpec as P

SPLIT = 4
CAP = 12
SLOTS = 16
CORES = 2
MESH = pl.DeviceIdType.MESH
BF = jnp.bfloat16
F32 = jnp.float32


def mm(a, b, ca=1, cb=0):
    return lax.dot_general(a, b, (((ca,), (cb,)), ((), ())), preferred_element_type=F32)


def kernel(
    n_s, n_e, n_d, steps,
    arr_h, fresh_h, routes_h, gates_h, cot_h, gain_h, wg_h, wu_h, wd_h,
    out, grad,
    out_v, grad_v, store_sems, fresh, routes, gates, cot, gain, wg, wu, wd, load_sems,
    toks, tokr, cots, cotr, parts, partr, hid, rets, pair, rsum, retr,
    base, inc, place_s, place_r, rows_s, rows_r,
    send_sems, recv_sems,
):
    sec = lax.axis_index("section")
    exp = lax.axis_index("expert")
    dp = lax.axis_index("dp")
    chips = n_e * n_d // CORES
    group = CORES * chips
    flight = n_e // SPLIT
    tok_rows, width = inc.shape[1:]
    cols = width // n_d
    half = cols // 2
    wide_cols = cols + half
    chunk = CAP * chips // n_d
    rows_half = CAP * chips
    used = flight * SLOTS
    compact = used < tok_rows
    core = lax.rem(exp, CORES)
    chip = (exp // CORES) * n_d + dp
    sibling = (sec, exp + 1 - 2 * core, dp)
    nxt = lax.rem(sec + 1, n_s)

    def far(j):
        low = n_d - 1 - j - (dp + j) // max(n_d - 1, 1)
        high = j + (j - dp + n_d) // n_d
        up = dp // ((n_d + 1) // 2)
        return up * high + (1 - up) * low

    n_y = n_e // CORES
    mine_y = exp // CORES

    def each(body):
        def far_one(i):
            body((mine_y + 1 + lax.rem(i, n_y)) % n_y, far(i // n_y))

        if chips <= 32:
            for i in range((n_d - 1) * n_y):
                body((mine_y + 1 + i % n_y) % n_y, far(i // n_y))
        else:
            @pl.loop(0, (n_d - 1) * n_y)
            def _(i):
                far_one(i)
        for o in range(1, n_y):
            body((mine_y + o) % n_y, dp)

    barrier = pltpu.get_barrier_semaphore()

    def signal(target):
        pl.semaphore_signal(barrier, inc=1, device_id=target, device_id_type=MESH)

    each(lambda ty, td: signal((sec, ty * CORES + core, td)))
    signal(sibling)
    greeted = chips
    for off in sorted({off for off in (1 % n_s, (n_s - 1) % n_s) if off}):
        signal((lax.rem(sec + off, n_s), exp, dp))
        greeted += 1

    loads = [
        pltpu.make_async_copy(src, dst, load_sems.at[i])
        for i, (src, dst) in enumerate((
            (routes_h, routes), (gates_h, gates), (gain_h, gain), (arr_h.at[0], inc.at[0]),
            (cot_h, cot), (wg_h, wg), (wu_h, wu), (wd_h, wd), (fresh_h, fresh),
        ))
    ]
    for load in loads:
        load.start()

    def remote(src, dst, k, phase, target):
        return pltpu.make_async_remote_copy(
            src_ref=src, dst_ref=dst, send_sem=send_sems.at[k, phase],
            recv_sem=recv_sems.at[k, phase], device_id=target, device_id_type=MESH,
        )

    def wait_all(ref, k, phase, send=False):
        copy = remote(ref, ref, k, phase, sibling)
        if send:
            copy.wait_send()
        else:
            copy.wait_recv()

    for load in loads[:3]:
        load.wait()

    lane = lax.broadcasted_iota(jnp.int32, (used, tok_rows), 0)
    lane_expert = lane >> 4
    lane_slot = lane & (SLOTS - 1)
    t_row = lax.broadcasted_iota(jnp.int32, (tok_rows, tok_rows), 0)
    t_col = lax.broadcasted_iota(jnp.int32, (tok_rows, tok_rows), 1)
    earlier_tok = jnp.where(t_row < t_col, 1.0, 0.0).astype(BF)

    def selection(k):
        naming = jnp.zeros((used, tok_rows), F32)
        shares = jnp.zeros((used, tok_rows), F32)
        for j in range(routes.shape[1]):
            hit = routes[0, j, k:k + 1, :] == lane_expert
            naming = jnp.where(hit, 1.0, naming)
            shares = shares + jnp.where(hit, gates[0, j].astype(F32)[k:k + 1, :], 0.0)
        places = mm(naming.astype(BF), earlier_tok)
        chosen = jnp.where(places == lane_slot.astype(F32), naming, 0.0)
        chosen = jnp.where(lane_slot < CAP, chosen, 0.0)
        slot_gate = jnp.sum(chosen * shares, axis=1, keepdims=True)
        return chosen.astype(BF), slot_gate

    picks = [selection(k) for k in range(steps)]

    r_i = lax.broadcasted_iota(jnp.int32, (CAP * chips, 8 * chips), 0)
    c_i = lax.broadcasted_iota(jnp.int32, (CAP * chips, 8 * chips), 1)
    c_slot = c_i & 7
    shift = r_i - (c_i >> 3) * CAP - c_slot
    low_rows = jnp.where(shift == 0, 1.0, 0.0).astype(BF)
    tail_a = jnp.where((shift == 8) & (c_slot < 4), 1.0, 0.0).astype(BF)
    tail_b = jnp.where((shift == 4) & (c_slot >= 4), 1.0, 0.0).astype(BF)

    def swap(block):
        return jnp.concatenate([block[4:], block[:4]], axis=0)

    def fill_rows(store, k, rows):
        for f in range(flight):
            top = rows[f * SLOTS:f * SLOTS + 8]
            bottom = rows[f * SLOTS + 8:(f + 1) * SLOTS]
            for d in range(n_d):
                at = d * cols
                store[k, d, f, :, :cols] = top[:, at:at + cols].astype(BF)
                store[k, d, f, :, cols:] = (
                    bottom[:, at:at + half] + swap(bottom[:, at + half:at + cols])
                ).astype(BF)

    def unpack(landing, k, part):
        flat = landing[k, part].reshape(chips * 8, wide_cols)
        tail = flat[:, cols:]
        return jnp.concatenate(
            [
                mm(low_rows, flat[:, :half]) + mm(tail_a, tail),
                mm(low_rows, flat[:, half:cols]) + mm(tail_b, tail),
            ],
            axis=1,
        ).astype(BF)

    def spread(store, landing, k, phase):
        def one(ty, td):
            te = ty * CORES + core
            remote(
                store.at[k, td, te // SPLIT], landing.at[k, core, chip], k, phase, (sec, te, td)
            ).start()

        each(one)
        landing[k, core, chip] = store[k, dp, exp // SPLIT]

    def pass_on(landing, k, phase):
        wait_all(landing.at[k, 0, pl.ds(0, chips - 1)], k, phase)
        remote(landing.at[k, core], landing.at[k, core], k, phase + 1, sibling).start()

    def load_in(k):
        return inc[k]

    def tok_phase(k):
        rows = mm(picks[k][0], load_in(k))
        scale = lax.rsqrt(jnp.mean(rows * rows, axis=1, keepdims=True) + 0.5)
        fill_rows(toks, k, rows * scale * gain[...])

    for k in range(steps):
        sel, slot_gate = picks[k]
        if k == 0:
            loads[3].wait()
        tok_phase(k)
        if k == 0:
            pl.semaphore_wait(barrier, greeted)
        spread(toks, tokr, k, 0)
        if n_s > 1 and compact and k < steps - 1:
            place_s[k] = sel
            remote(place_s.at[k], place_r.at[k], k, 8, (nxt, exp, dp)).start()
            remote(inc.at[k], base.at[k], k, 9, (nxt, exp, dp)).start()
        if k == 0:
            loads[4].wait()
            for turn in range(steps):
                pick, share = picks[turn]
                fill_rows(cots, turn, mm(pick, cot[0, turn]) * share)
                spread(cots, cotr, turn, 2)

        pass_on(tokr, k, 0)
        if k == 0:
            for load in loads[5:]:
                load.wait()

        def partial_sums(part, phase):
            tok = unpack(tokr, k, part)
            for i, weight in enumerate((wg, wu)):
                acted = mm(tok, weight[0], 1, 1)
                for d in range(n_d):
                    parts[k, part, d, i] = acted[d * chunk:(d + 1) * chunk].astype(BF)
            for j in range(n_d - 1):
                td = far(j) if phase == 11 else lax.rem(dp + 1 + j, n_d)
                remote(
                    parts.at[k, part, td], partr.at[k, part, dp], k, phase, (sec, exp, td)
                ).start()
            partr[k, part, dp] = parts[k, part, dp]

        def activate(part, phase):
            wait_all(partr.at[k, 0, pl.ds(0, n_d - 1)], k, phase)
            act_g = sum(partr[k, part, d, 0].astype(F32) for d in range(n_d))
            act_u = sum(partr[k, part, d, 1].astype(F32) for d in range(n_d))
            hid[k, part, dp] = (act_g / (1.0 + jnp.exp(-act_g)) * act_u).astype(BF)
            for j in range(n_d - 1):
                mine = hid.at[k, part, dp]
                remote(mine, mine, k, phase + 1, (sec, exp, far(j))).start()

        def down(part, phase):
            wait_all(hid.at[k, 0, pl.ds(0, n_d - 1)], k, phase + 1)
            hidden = hid[k, part].reshape(rows_half, wg.shape[1])
            piece = mm(hidden, wd[0]).astype(BF)
            rets[k, part, :, :, :cols] = mm(low_rows, piece, 0, 0).astype(BF).reshape(
                chips, 8, cols
            )
            rets[k, part, :, :, cols:] = (
                mm(tail_a, piece[:, :half], 0, 0) + mm(tail_b, piece[:, half:], 0, 0)
            ).astype(BF).reshape(chips, 8, half)

        partial_sums(core, 4)
        wait_all(tokr.at[k, 0], k, 1)
        partial_sums(1 - core, 11)
        pass_on(cotr, k, 2)
        activate(core, 4)
        activate(1 - core, 11)
        down(core, 4)
        down(1 - core, 11)

        remote(rets.at[k, 1 - core], pair.at[k], k, 6, sibling).start()
        wait_all(pair.at[k], k, 6)
        rsum[k] = (rets[k, core].astype(F32) + pair[k].astype(F32)).astype(BF)

        def give_back(ty, td):
            remote(
                rsum.at[k, ty * n_d + td], retr.at[k, mine_y, dp], k, 7,
                (sec, ty * CORES + core, td),
            ).start()

        each(give_back)
        retr[k, exp // CORES, dp] = rsum[k, chip]
        wait_all(cotr.at[k, 0], k, 3)
        part = sum(
            mm(hid[k, c].reshape(rows_half, wg.shape[1]), unpack(cotr, k, c), 0, 0)
            for c in range(CORES)
        )
        grad_v[...] = part if k == 0 else grad_v[...] + part
        if k == steps - 1:
            pltpu.make_async_copy(grad_v, grad.at[0], store_sems.at[steps]).start()

        wait_all(rsum.at[k, pl.ds(0, chips - 1)], k, 7)
        tops = []
        row_8 = lax.broadcasted_iota(jnp.int32, (8, half), 0)
        pairs = SPLIT // CORES
        for f in range(flight):
            top, tail = [], []
            for d in range(n_d):
                total = sum(retr[k, f * pairs + j, d].astype(F32) for j in range(pairs))
                top.append(total[:, :cols])
                last = total[:, cols:]
                tail.append(jnp.where(row_8 < 4, last, 0.0))
                tail.append(jnp.where(row_8 < 4, swap(last), 0.0))
            tops.append(jnp.concatenate(top, axis=1))
            tops.append(jnp.concatenate(tail, axis=1))
        mixed = jnp.concatenate(tops, axis=0) * slot_gate
        high = mixed.astype(BF)
        low = (mixed - high.astype(F32)).astype(BF)
        mixture = mm(sel, high, 0, 0) + mm(sel, low, 0, 0)
        result = (load_in(k).astype(F32) + mixture).astype(BF)
        out_v[k] = result
        pltpu.make_async_copy(out_v.at[k], out.at[0, k], store_sems.at[k]).start()
        if k + 1 < steps:
            if n_s == 1:
                inc[k + 1] = fresh[k]
            elif compact:
                rows_s[k] = mm(sel, result).astype(BF)
                remote(rows_s.at[k], rows_r.at[k], k, 10, (nxt, exp, dp)).start()
                wait_all(base.at[k], k, 9)
                wait_all(place_r.at[k], k, 8)
                wait_all(rows_r.at[k], k, 10)
                spot = place_r[k]
                if flight > 1:
                    u_row = lax.broadcasted_iota(jnp.int32, (used, used), 0) >> 4
                    u_col = lax.broadcasted_iota(jnp.int32, (used, used), 1) >> 4
                    sooner = jnp.where(u_col < u_row, 1.0, 0.0).astype(BF)
                    spot = jnp.where(mm(sooner, spot) > 0.5, 0.0, spot.astype(F32)).astype(BF)
                kept = mm(spot, jnp.ones((used, width), BF), 0, 0)
                moved = jnp.where(kept > 0.5, mm(spot, rows_r[k], 0, 0), base[k].astype(F32))
                inc[k + 1] = jnp.where(sec == 0, fresh[k].astype(F32), moved).astype(BF)
            else:
                remote(out_v.at[k], base.at[k], k, 9, (nxt, exp, dp)).start()
                wait_all(base.at[k], k, 9)
                inc[k + 1] = jnp.where(
                    sec == 0, fresh[k].astype(F32), base[k].astype(F32)
                ).astype(BF)

    pltpu.make_async_copy(grad_v, grad.at[0], store_sems.at[steps]).wait()
    for k in range(steps):
        wait_all(tokr.at[k, 0, pl.ds(0, chips - 1)], k, 0, True)
        pltpu.make_async_copy(out_v.at[k], out.at[0, k], store_sems.at[k]).wait()
        wait_all(tokr.at[k, 0], k, 1, True)
        wait_all(cotr.at[k, 0, pl.ds(0, chips - 1)], k, 2, True)
        wait_all(cotr.at[k, 0], k, 3, True)
        for phase in (4, 11):
            wait_all(parts.at[k, 0, pl.ds(0, n_d - 1)], k, phase, True)
            wait_all(hid.at[k, 0, pl.ds(0, n_d - 1)], k, phase + 1, True)
        wait_all(pair.at[k], k, 6, True)
        wait_all(rsum.at[k, pl.ds(0, chips - 1)], k, 7, True)
        if n_s > 1 and k < steps - 1:
            wait_all(base.at[k], k, 9, True)
            if compact:
                wait_all(place_s.at[k], k, 8, True)
                wait_all(rows_s.at[k], k, 10, True)


def finish(out_in, grad_in, out, grad, out_v, grad_v, in_sems, out_sems):
    steps, tok_rows = out_v.shape[1:3]
    units = grad_v.shape[1]
    moves = []
    for k in range(steps):
        for h in range(2):
            part = (0, k, pl.ds(h * tok_rows // 2, tok_rows // 2))
            moves.append((out_in.at[part], out_v.at[part], out.at[part]))
    for h in range(4):
        part = (0, pl.ds(h * units // 4, units // 4))
        moves.append((grad_in.at[part], grad_v.at[part], grad.at[part]))
    loads = [
        pltpu.make_async_copy(src, held, in_sems.at[i]) for i, (src, held, _) in enumerate(moves)
    ]
    stores = [
        pltpu.make_async_copy(held, dst, out_sems.at[i]) for i, (_, held, dst) in enumerate(moves)
    ]
    for load in loads:
        load.start()
    for load, store in zip(loads, stores):
        load.wait()
        store.start()
    for store in stores:
        store.wait()


def local(sizes, arrivals, fresh, routes, gates, cotangent, norm_gain, w_gate, w_up, w_down):
    n_s, n_e, n_d = sizes
    steps = routes.shape[1]
    tok_rows, width = arrivals.shape[1:]
    units, cols = w_gate.shape[1:]
    flight = n_e // SPLIT
    chips = n_e * n_d // CORES
    chunk = CAP * chips // n_d
    used = flight * SLOTS
    hops = max(steps - 1, 1)
    packed = cols + cols // 2
    hbm = pl.BlockSpec(memory_space=pltpu.HBM)
    made = pl.pallas_call(
        functools.partial(kernel, n_s, n_e, n_d, steps),
        out_shape=(
            jax.ShapeDtypeStruct((1, steps, tok_rows, width), BF),
            jax.ShapeDtypeStruct((1, units, cols), F32),
        ),
        in_specs=[hbm] * 9,
        out_specs=(hbm, hbm),
        scratch_shapes=[
            pltpu.VMEM((steps, tok_rows, width), BF),
            pltpu.VMEM((units, cols), F32),
            pltpu.SemaphoreType.DMA((steps + 1,)),
            pltpu.VMEM(fresh.shape, BF),
            pltpu.VMEM((1, routes.shape[3], steps, tok_rows), jnp.int32),
            pltpu.VMEM((1, routes.shape[3], steps, tok_rows), BF),
            pltpu.VMEM(cotangent.shape, BF),
            pltpu.VMEM(norm_gain.shape, F32),
            pltpu.VMEM(w_gate.shape, BF),
            pltpu.VMEM(w_up.shape, BF),
            pltpu.VMEM(w_down.shape, BF),
            pltpu.SemaphoreType.DMA((9,)),
            pltpu.VMEM((steps, n_d, flight, 8, packed), BF),
            pltpu.VMEM((steps, CORES, chips, 8, packed), BF),
            pltpu.VMEM((steps, n_d, flight, 8, packed), BF),
            pltpu.VMEM((steps, CORES, chips, 8, packed), BF),
            pltpu.VMEM((steps, CORES, n_d, 2, chunk, units), BF),
            pltpu.VMEM((steps, CORES, n_d, 2, chunk, units), BF),
            pltpu.VMEM((steps, CORES, n_d, chunk, units), BF),
            pltpu.VMEM((steps, CORES, chips, 8, packed), BF),
            pltpu.VMEM((steps, chips, 8, packed), BF),
            pltpu.VMEM((steps, chips, 8, packed), BF),
            pltpu.VMEM((steps, n_e // CORES, n_d, 8, packed), BF),
            pltpu.VMEM((hops, tok_rows, width), BF),
            pltpu.VMEM((steps, tok_rows, width), BF),
            pltpu.VMEM((hops, used, tok_rows), BF),
            pltpu.VMEM((hops, used, tok_rows), BF),
            pltpu.VMEM((hops, used, width), BF),
            pltpu.VMEM((hops, used, width), BF),
            pltpu.SemaphoreType.DMA((steps, 13)),
            pltpu.SemaphoreType.DMA((steps, 13)),
        ],
        compiler_params=pltpu.CompilerParams(
            collective_id=0, has_side_effects=True, vmem_limit_bytes=60000 * 1024
        ),
    )(
        arrivals, fresh, jnp.transpose(routes, (0, 3, 1, 2)),
        jnp.transpose(gates, (0, 3, 1, 2)), cotangent,
        norm_gain, w_gate, w_up, w_down,
    )
    pieces = steps * 2 + 4
    return pl.pallas_call(
        finish,
        out_shape=tuple(jax.ShapeDtypeStruct(m.shape, m.dtype) for m in made),
        in_specs=[hbm] * 2,
        out_specs=(hbm, hbm),
        scratch_shapes=[pltpu.VMEM(m.shape, m.dtype) for m in made]
        + [pltpu.SemaphoreType.DMA((pieces,)), pltpu.SemaphoreType.DMA((pieces,))],
        compiler_params=pltpu.CompilerParams(vmem_limit_bytes=60000 * 1024),
    )(*made)


def solution(mesh):
    placed = (
        P("section", ("expert", "dp"), None),
        P(None, ("expert", "dp"), None),
        P("section", None, ("expert", "dp"), None),
        P("section", None, ("expert", "dp"), None),
        P("section", None, ("expert", "dp"), None),
        P("section", None),
        P("section", "expert", "dp"),
        P("section", "expert", "dp"),
        P("section", "expert", "dp"),
    )
    sizes = (mesh.shape["section"], mesh.shape["expert"], mesh.shape["dp"])
    return jax.shard_map(
        functools.partial(local, sizes),
        mesh=mesh,
        in_specs=placed,
        out_specs=(P("section", None, ("expert", "dp"), None), P("section", "expert", "dp")),
        check_vma=False,
    )
```
